32 devices in a mesh: rep: 2 (over x), tp: 4 (over z), sp: 4 (over y, core).
Axes of the slice: x: 2, y: 2, z: 4, core: 2. Of those that a mesh axis runs over, the one named last changes fastest.
Arguments:
- x_tokens: bfloat16 [8192, 2560], P(('rep', 'sp')), parts along dimension 0
- positions: int32 [8192], P(('rep', 'sp')), parts along dimension 0
- gains: float32 [2, 4, 2560], replicated
- w_q: bfloat16 [2, 2560, 32, 128], P(None, None, 'tp')
- w_k: bfloat16 [2, 2560, 8, 128], P(None, None, 'tp')
- w_v: bfloat16 [2, 2560, 8, 128], P(None, None, 'tp')
- w_o: bfloat16 [2, 32, 128, 2560], P(None, 'tp')
- w_gate: bfloat16 [2, 2560, 9728], P(None, None, 'tp')
- w_up: bfloat16 [2, 2560, 9728], P(None, None, 'tp')
- w_down: bfloat16 [2, 9728, 2560], P(None, 'tp')
Outputs:
- output 1: bfloat16 [8192, 2560], P(('rep', 'sp')), parts along dimension 0
- output 2: bfloat16 [1024, 16, 128], P('rep', ('tp', 'sp')), parts along dimension 0
- output 3: bfloat16 [1024, 16, 128], P('rep', ('tp', 'sp')), parts along dimension 0
- output 4: bfloat16 [8192, 16, 128], P('rep', ('tp', 'sp')), parts along dimension 0
- output 5: bfloat16 [8192, 16, 128], P('rep', ('tp', 'sp')), parts along dimension 0
There are 2 independent parts. The reference program is written for one: setup_inputs(seed, part) draws one part's arguments, and reference() takes and returns one part's arrays. A program takes and returns all parts, laid end to end along the dimension named above; an argument that names none is the same for every part.
All inputs are finite; a program needn't handle non-finite values.
Results may differ from the reference program's by a relative error of at most 0.0160804.
Values are sent between devices in bfloat16 or wider.
A program may use at most 1 GiB of HBM per device.

```python
import jax
import jax.numpy as jnp
from jax import lax

D = 2560
HEADS = 32
KV_HEADS = 8
HEAD = 128
FF = 9728
TOKENS = 4096
WINDOW = 512
CACHE_HEADS = 16
REF_BLOCK = 64

GROUP_SIZE = HEADS // KV_HEADS
REPEAT = CACHE_HEADS // KV_HEADS
NORM_EPS = 1e-6
LOCAL_BASE = 10000.0
GLOBAL_BASE = 1000000.0


def setup_inputs(seed: int = 0, part: int = 0) -> dict:
    part_key = jax.random.fold_in(jax.random.key(seed), part)
    key_x, key_pos = jax.random.split(part_key, 2)
    weight_keys = jax.random.split(jax.random.key(seed + 1), 8)
    x_tokens = jax.random.normal(key_x, (TOKENS, D), jnp.float32).astype(jnp.bfloat16)
    start = jax.random.randint(key_pos, (), 0, 4096)
    positions = (start + jnp.arange(TOKENS)).astype(jnp.int32)
    gains = 1.0 + 0.25 * jax.random.normal(weight_keys[0], (2, 4, D), jnp.float32)

    def weight(key, shape, fan_in):
        return (jax.random.normal(key, shape, jnp.float32) * fan_in ** -0.5).astype(jnp.bfloat16)

    return {
        'x_tokens': x_tokens,
        'positions': positions,
        'gains': gains,
        'w_q': weight(weight_keys[1], (2, D, HEADS, HEAD), D),
        'w_k': weight(weight_keys[2], (2, D, KV_HEADS, HEAD), D),
        'w_v': weight(weight_keys[3], (2, D, KV_HEADS, HEAD), D),
        'w_o': weight(weight_keys[4], (2, HEADS, HEAD, D), HEADS * HEAD),
        'w_gate': weight(weight_keys[5], (2, D, FF), D),
        'w_up': weight(weight_keys[6], (2, D, FF), D),
        'w_down': weight(weight_keys[7], (2, FF, D), FF),
    }


def rms_norm(values, gain):
    wide = values.astype(jnp.float32)
    inv_rms = lax.rsqrt(jnp.mean(wide * wide, axis=-1, keepdims=True) + NORM_EPS)
    return wide * inv_rms * gain


def rotary(projected, positions, base):
    half = projected.shape[-1] // 2
    inv_freq = base ** (-jnp.arange(half, dtype=jnp.float32) / half)
    angles = positions.astype(jnp.float32)[..., None] * inv_freq
    cos_part = jnp.cos(angles)[..., None, :]
    sin_part = jnp.sin(angles)[..., None, :]
    first = projected[..., :half]
    second = projected[..., half:]
    return jnp.concatenate([first * cos_part - second * sin_part, second * cos_part + first * sin_part], axis=-1)


def attention(q_rot, k_rot, v_new, local):
    q_wide = q_rot.reshape(TOKENS, KV_HEADS, GROUP_SIZE, HEAD).astype(jnp.float32)
    k_wide = k_rot.astype(jnp.float32)
    v_wide = v_new.astype(jnp.float32)
    span = WINDOW + REF_BLOCK if local else TOKENS

    def one_block(block_id):
        q_start = block_id * REF_BLOCK
        q_tile = lax.dynamic_slice_in_dim(q_wide, q_start, REF_BLOCK, 0)
        q_idx = q_start + jnp.arange(REF_BLOCK)
        k_start = jnp.clip(q_start - WINDOW, 0, TOKENS - span) if local else 0
        k_tile = lax.dynamic_slice_in_dim(k_wide, k_start, span, 0)
        v_tile = lax.dynamic_slice_in_dim(v_wide, k_start, span, 0)
        k_idx = k_start + jnp.arange(span)
        allowed = k_idx[None, :] <= q_idx[:, None]
        if local:
            allowed = allowed & (q_idx[:, None] - k_idx[None, :] < WINDOW)
        scores = jnp.einsum('qhgd,khd->hgqk', q_tile, k_tile) * (HEAD ** -0.5)
        weights = jax.nn.softmax(jnp.where(allowed, scores, -1e30), axis=-1)
        weights = weights.astype(jnp.bfloat16).astype(jnp.float32)
        return jnp.einsum('hgqk,khd->qhgd', weights, v_tile).astype(jnp.bfloat16)

    blocks = lax.map(one_block, jnp.arange(TOKENS // REF_BLOCK))
    return blocks.reshape(TOKENS, HEADS * HEAD)


def layer(hidden, positions, gain, w_q, w_k, w_v, w_o, w_gate, w_up, w_down, local):
    base = LOCAL_BASE if local else GLOBAL_BASE
    u_norm = rms_norm(hidden, gain[0]).astype(jnp.bfloat16)
    q_proj = jnp.dot(u_norm, w_q.reshape(D, HEADS * HEAD), preferred_element_type=jnp.float32)
    k_proj = jnp.dot(u_norm, w_k.reshape(D, KV_HEADS * HEAD), preferred_element_type=jnp.float32)
    v_proj = jnp.dot(u_norm, w_v.reshape(D, KV_HEADS * HEAD), preferred_element_type=jnp.float32)
    q_rot = rotary(q_proj.reshape(TOKENS, HEADS, HEAD), positions, base).astype(jnp.bfloat16)
    k_rot = rotary(k_proj.reshape(TOKENS, KV_HEADS, HEAD), positions, base).astype(jnp.bfloat16)
    v_new = v_proj.reshape(TOKENS, KV_HEADS, HEAD).astype(jnp.bfloat16)
    attn_out = attention(q_rot, k_rot, v_new, local)
    o_sum = jnp.dot(attn_out, w_o.reshape(HEADS * HEAD, D), preferred_element_type=jnp.float32)
    x_mid = (hidden.astype(jnp.float32) + rms_norm(o_sum, gain[1])).astype(jnp.bfloat16)
    u_mlp = rms_norm(x_mid, gain[2]).astype(jnp.bfloat16)
    gate_pre = jnp.dot(u_mlp, w_gate, preferred_element_type=jnp.float32)
    up_pre = jnp.dot(u_mlp, w_up, preferred_element_type=jnp.float32)
    hidden_act = (jax.nn.silu(gate_pre) * up_pre).astype(jnp.bfloat16)
    m_sum = jnp.dot(hidden_act, w_down, preferred_element_type=jnp.float32)
    x_out = (x_mid.astype(jnp.float32) + rms_norm(m_sum, gain[3])).astype(jnp.bfloat16)
    k_cache = jnp.repeat(k_rot, REPEAT, axis=1)
    v_cache = jnp.repeat(v_new, REPEAT, axis=1)
    if local:
        return x_out, k_cache[TOKENS - WINDOW:], v_cache[TOKENS - WINDOW:]
    return x_out, k_cache, v_cache


def reference(x_tokens, positions, gains, w_q, w_k, w_v, w_o, w_gate, w_up, w_down):
    hidden, k_local, v_local = layer(x_tokens, positions, gains[0], w_q[0], w_k[0], w_v[0], w_o[0], w_gate[0], w_up[0], w_down[0], True)
    out_hidden, k_global, v_global = layer(hidden, positions, gains[1], w_q[1], w_k[1], w_v[1], w_o[1], w_gate[1], w_up[1], w_down[1], False)
    return out_hidden, k_local, v_local, k_global, v_global
```

```python
import functools
import jax
import jax.numpy as jnp
from jax import lax
from jax.experimental import pallas as pl
from jax.experimental.pallas import tpu as pltpu
from jax.sharding import PartitionSpec as P

MESH = pl.DeviceIdType.MESH
NORM_EPS = 1e-6
D = 2560
WINDOW = 512
QB = 256
LOG2E = 1.4426950408889634
NT = (((1,), (1,)), ((), ()))

def attn_kernel(local, x_hbm, g_ref, cos_ref, sin_ref, wkv_hbm, wq_hbm, a_hbm, kc_hbm, vc_hbm,
                x_v, wkv_v, wq_v, q_v, kv, cache, m_v, l_v, acc_v, a_v,
                w_sem, ps_sem, pr_sem, ys_sem, yr_sem, fs_sem, fr_sem, c_sem):
    s = lax.axis_index('sp')
    rows = x_v.shape[0]
    nq = rows // QB
    y = s // 2
    pair = {'sp': s + 1 - 2 * lax.rem(s, 2)}
    across = {'sp': lax.rem(s + 2, 4)}
    loads = [pltpu.make_async_copy(x_hbm, x_v, w_sem.at[0]), pltpu.make_async_copy(wkv_hbm, wkv_v, w_sem.at[1]),
             pltpu.make_async_copy(wq_hbm, wq_v, w_sem.at[2])]
    for c in loads:
        c.start()
    bar = pltpu.get_barrier_semaphore()
    if local:
        own = WINDOW

        @pl.when(s > 0)
        def _():
            pl.semaphore_signal(bar, inc=1, device_id={'sp': jnp.maximum(s - 1, 0)}, device_id_type=MESH)

        @pl.when(s < 3)
        def _():
            pl.semaphore_signal(bar, inc=1, device_id={'sp': 3}, device_id_type=MESH)
        pl.semaphore_wait(bar, jnp.where(s == 3, 3, 1))
    else:
        own = pl.multiple_of(s * rows, rows)
        for peer in (pair, across):
            pl.semaphore_signal(bar, inc=1, device_id=peer, device_id_type=MESH)
        pl.semaphore_wait(bar, 2)

    def halo():
        return pltpu.make_async_remote_copy(kv.at[:, pl.ds(rows, WINDOW), :], kv.at[:, pl.ds(0, WINDOW), :],
                                            ps_sem.at[0], pr_sem.at[0], device_id={'sp': jnp.minimum(s + 1, 3)}, device_id_type=MESH)

    def tail(dst, kind):
        return pltpu.make_async_remote_copy(kv.at[2 * kind + dst // 2, pl.ds(rows, WINDOW), :], cache.at[kind],
                                            ys_sem.at[dst, kind], yr_sem.at[kind], device_id={'sp': dst}, device_id_type=MESH)

    def region(b):
        return kv.at[:, pl.ds(pl.multiple_of(own + b * QB, QB), QB), :]

    def to_pair(b):
        return pltpu.make_async_remote_copy(region(b), region(b), ps_sem.at[b], pr_sem.at[b], device_id=pair, device_id_type=MESH)

    def to_across(b):
        return pltpu.make_async_remote_copy(region(b), region(b), ys_sem.at[b], yr_sem.at[b], device_id=across, device_id_type=MESH)

    def fwd(b):
        ref = kv.at[:, pl.ds(pl.multiple_of(lax.rem(s + 2, 4) * rows + b * QB, QB), QB), :]
        return pltpu.make_async_remote_copy(ref, ref, fs_sem.at[b], fr_sem.at[b], device_id=pair, device_id_type=MESH)

    def rope(v, rs):
        return v * cos_ref[rs, :] + pltpu.roll(v, 64, 1) * sin_ref[rs, :]

    loads[0].wait()
    loads[1].wait()

    def kv_block(k, _):
        b = lax.rem(k + 2, nq) if local else k
        rs = pl.ds(pl.multiple_of(b * QB, QB), QB)
        wide = x_v[rs, :].astype(jnp.float32)
        u = (wide * lax.rsqrt(jnp.mean(wide * wide, axis=-1, keepdims=True) + NORM_EPS) * g_ref[0:1, :]).astype(jnp.bfloat16)
        x_v[rs, :] = u
        p = jnp.dot(u, wkv_v[...], preferred_element_type=jnp.float32)
        dst = pl.ds(pl.multiple_of(own + b * QB, QB), QB)
        for h in range(2):
            kv[h, dst, :] = rope(p[:, h * 128:(h + 1) * 128], rs).astype(jnp.bfloat16)
            kv[2 + h, dst, :] = p[:, (2 + h) * 128:(3 + h) * 128].astype(jnp.bfloat16)
        if local:
            @pl.when(k == 1)
            def _():
                @pl.when(s < 3)
                def _():
                    halo().start()

                @pl.when(s == 3)
                def _():
                    for dst in range(3):
                        for kind in range(2):
                            tail(dst, kind).start()
        else:
            to_across(b).start()
            to_pair(b).start()
        return 0
    lax.fori_loop(0, nq, kv_block, 0)

    loads[2].wait()

    def q_block(b, _):
        rs = pl.ds(pl.multiple_of(b * QB, QB), QB)
        for g in range(2):
            for hh in range(2):
                p = jnp.dot(x_v[rs, :], wq_v[:, (g * 4 + hh * 2) * 128:(g * 4 + hh * 2 + 2) * 128], preferred_element_type=jnp.float32)
                for e in range(2):
                    q_v[g, b, hh, pl.ds(e * QB, QB), :] = rope(p[:, e * 128:(e + 1) * 128], rs).astype(jnp.bfloat16)
        return 0
    lax.fori_loop(0, nq, q_block, 0)

    scale = 128 ** -0.5 * LOG2E

    def scores(g, b, hh, ks):
        return lax.dot_general(q_v[g, b, hh], kv[g, ks, :], NT, preferred_element_type=jnp.float32) * scale

    def emit(g, b, hh, o):
        for e in range(2):
            a_v[pl.ds(pl.multiple_of(b * QB, QB), QB), pl.ds(pl.multiple_of((g * 4 + hh * 2 + e) * 128, 128), 128)] = o[e * QB:(e + 1) * QB]

    def tiles(fn):
        def body(k, _):
            fn(k // (2 * nq), lax.rem(k // 2, nq), lax.rem(k, 2))
            return 0
        lax.fori_loop(0, 4 * nq, body, 0)

    if local:
        @pl.when(s > 0)
        def _():
            halo().wait_recv()

        @pl.when(s == 0)
        def _():
            kv[:, :WINDOW, :] = jnp.zeros((4, WINDOW, 128), jnp.bfloat16)

        def tile(g, b, hh):
            span = WINDOW + QB
            ks = pl.ds(pl.multiple_of(b * QB, QB), span)
            sc = scores(g, b, hh, ks)
            i = lax.rem(lax.broadcasted_iota(jnp.int32, sc.shape, 0), QB)
            j = lax.broadcasted_iota(jnp.int32, sc.shape, 1)
            first = jnp.where(s == 0, WINDOW - b * QB, 0)
            ok = (j > i) & (j <= i + WINDOW) & (j >= first)
            sc = jnp.where(ok, sc, -1e30)
            p = jnp.exp2(sc - jnp.max(sc, axis=1, keepdims=True))
            o = jnp.dot(p.astype(jnp.bfloat16), kv[2 + g, ks, :], preferred_element_type=jnp.float32)
            emit(g, b, hh, (o / jnp.sum(p, axis=1, keepdims=True)).astype(jnp.bfloat16))
        tiles(tile)

        @pl.when(s < 3)
        def _():
            halo().wait_send()
            for kind in range(2):
                tail(0, kind).wait_recv()

        @pl.when(s == 3)
        def _():
            for dst in range(3):
                for kind in range(2):
                    tail(dst, kind).wait_send()
            for kind in range(2):
                cache[kind] = kv[2 * kind + 1, pl.ds(rows, WINDOW), :]
        outs = [pltpu.make_async_copy(a_v, a_hbm, c_sem.at[0]), pltpu.make_async_copy(cache.at[0], kc_hbm, c_sem.at[1]),
                pltpu.make_async_copy(cache.at[1], vc_hbm, c_sem.at[2])]
        for c in outs:
            c.start()
        for c in outs:
            c.wait()
        return

    def update(g, b, hh, ks, mask):
        sc = scores(g, b, hh, ks)
        if mask is not None:
            sc = jnp.where(mask(sc.shape), sc, -1e30)
        m_old = m_v[g, b, hh]
        m_new = jnp.maximum(m_old, jnp.max(sc, axis=1, keepdims=True))
        alpha = jnp.exp2(m_old - m_new)
        p = jnp.exp2(sc - jnp.concatenate([m_new] * (sc.shape[1] // 128), axis=1))
        part = p[:, :128]
        for c in range(1, sc.shape[1] // 128):
            part = part + p[:, c * 128:(c + 1) * 128]
        l_v[g, b, hh] = l_v[g, b, hh] * alpha + part
        acc_v[g, b, hh] = acc_v[g, b, hh] * alpha + jnp.dot(p.astype(jnp.bfloat16), kv[2 + g, ks, :], preferred_element_type=jnp.float32)
        m_v[g, b, hh] = m_new

    def diag(g, b, hh):
        m_v[g, b, hh] = jnp.full((2 * QB, 128), -1e30, jnp.float32)
        l_v[g, b, hh] = jnp.zeros((2 * QB, 128), jnp.float32)
        acc_v[g, b, hh] = jnp.zeros((2 * QB, 128), jnp.float32)

        def before(j, _):
            update(g, b, hh, pl.ds(pl.multiple_of(own + j * QB, QB), QB), None)
            return 0
        lax.fori_loop(0, b, before, 0)

        def mask(shape):
            return lax.broadcasted_iota(jnp.int32, shape, 1) <= lax.rem(lax.broadcasted_iota(jnp.int32, shape, 0), QB)
        update(g, b, hh, pl.ds(pl.multiple_of(own + b * QB, QB), QB), mask)
    tiles(diag)

    def full(src):
        def tile(g, b, hh):
            def blk(j, _):
                update(g, b, hh, pl.ds(pl.multiple_of(src * rows + j * 512, 512), 512), None)
                return 0
            lax.fori_loop(0, rows // 512, blk, 0)
        tiles(tile)

    def pass_on(b, _):
        to_across(b).wait_recv()
        fwd(b).start()
        return 0

    def wait_pair(b, _):
        to_pair(b).wait_recv()
        return 0

    def wait_fwd(b, _):
        fwd(b).wait_recv()
        return 0
    lax.fori_loop(0, nq, wait_pair, 0)

    @pl.when(lax.rem(s, 2) == 1)
    def _():
        full(s - 1)
    lax.fori_loop(0, nq, pass_on, 0)

    @pl.when(y == 1)
    def _():
        full(lax.rem(s + 2, 4))
    lax.fori_loop(0, nq, wait_fwd, 0)
    outs = [pltpu.make_async_copy(kv.at[y], kc_hbm, c_sem.at[1]), pltpu.make_async_copy(kv.at[2 + y], vc_hbm, c_sem.at[2])]
    for c in outs:
        c.start()

    @pl.when(y == 1)
    def _():
        full(1 - lax.rem(s, 2))

    def fin(g, b, hh):
        emit(g, b, hh, (acc_v[g, b, hh] / jnp.sum(l_v[g, b, hh], axis=1, keepdims=True)).astype(jnp.bfloat16))
    tiles(fin)
    last = pltpu.make_async_copy(a_v, a_hbm, c_sem.at[0])
    last.start()

    def sent(b, _):
        to_pair(b).wait_send()
        to_across(b).wait_send()
        fwd(b).wait_send()
        return 0
    lax.fori_loop(0, nq, sent, 0)
    for c in outs + [last]:
        c.wait()


def attn(local, x, gains, cos, sin, wkv, wq, cid):
    t = x.shape[0]
    nq = t // QB
    any_ = pl.BlockSpec(memory_space=pl.ANY)
    vm = pl.BlockSpec(memory_space=pltpu.VMEM)
    bf, f32 = jnp.bfloat16, jnp.float32
    dma = pltpu.SemaphoreType.DMA
    total = WINDOW if local else 4 * t
    kvrows = WINDOW + t if local else 4 * t
    st = (2, nq, 2, 2 * QB, 128) if not local else (1, 1, 1, 8, 128)
    return pl.pallas_call(
        functools.partial(attn_kernel, local),
        out_shape=[jax.ShapeDtypeStruct((t, 1024), bf), jax.ShapeDtypeStruct((total, 128), bf), jax.ShapeDtypeStruct((total, 128), bf)],
        in_specs=[any_, vm, vm, vm, any_, any_],
        out_specs=[any_, any_, any_],
        scratch_shapes=[
            pltpu.VMEM((t, D), bf), pltpu.VMEM((D, 512), bf), pltpu.VMEM((D, 1024), bf), pltpu.VMEM((2, nq, 2, 2 * QB, 128), bf),
            pltpu.VMEM((4, kvrows, 128), bf), pltpu.VMEM((2, WINDOW, 128), bf),
            pltpu.VMEM(st, f32), pltpu.VMEM(st, f32), pltpu.VMEM(st, f32), pltpu.VMEM((t, 1024), bf),
            dma((3,)), dma((nq,)), dma((nq,)), dma((3, 2)) if local else dma((nq,)), dma((2,)) if local else dma((nq,)),
            dma((nq,)), dma((nq,)), dma((3,))],
        compiler_params=pltpu.CompilerParams(collective_id=cid, has_side_effects=True, vmem_limit_bytes=60 * 2**20),
        cost_estimate=pl.CostEstimate(flops=20_000_000_000, bytes_accessed=20_000_000, transcendentals=10_000_000),
        name='attn_local' if local else 'attn_global',
    )(x, gains, cos, sin, wkv, wq)


def ffn_kernel(layer, C, a_hbm, h_hbm, g_ref, wo_hbm, wg_hbm, wu_hbm, wd_hbm, out_hbm,
               wo_v, wg_v, wu_v, wd_v, a_v, hb, ub, so, sm, ro, rm, lhs_a, lhs_u, fb,
               w_sem, os_sem, or_sem, ms_sem, mr_sem, us_sem, ur_sem, hs_sem, hr_sem, out_sem):
    z = lax.axis_index('tp')
    half = a_hbm.shape[0] // 2
    n = half // C
    q = ro.shape[1]
    ff = wg_v.shape[1]
    r = (z, 3 - z)
    toward = ({'tp': jnp.maximum(z - 1, 0)}, {'tp': jnp.minimum(z + 1, 3)})
    away = ({'tp': jnp.minimum(z + 1, 3)}, {'tp': jnp.maximum(z - 1, 0)})

    def load(k, src, dst):
        return pltpu.make_async_copy(src, dst, w_sem.at[k])

    is_end = (z == 0) | (z == 3)
    loads = [load(0, wo_hbm.at[layer], wo_v), load(1, a_hbm, a_v), load(2, wg_hbm.at[layer], wg_v),
             load(3, wu_hbm.at[layer], wu_v), load(4, wd_hbm.at[layer], wd_v)]
    res = load(5, h_hbm.at[pl.ds(pl.multiple_of(jnp.where(z == 3, half, 0), half), half), :], hb)
    for c in loads[:2]:
        c.start()

    @pl.when(is_end)
    def _():
        res.start()
    for c in loads[2:]:
        c.start()

    bar = pltpu.get_barrier_semaphore()

    @pl.when(z > 0)
    def _():
        pl.semaphore_signal(bar, inc=1, device_id={'tp': jnp.maximum(z - 1, 0)}, device_id_type=MESH)

    @pl.when(z < 3)
    def _():
        pl.semaphore_signal(bar, inc=1, device_id={'tp': jnp.minimum(z + 1, 3)}, device_id_type=MESH)
    pl.semaphore_wait(bar, jnp.where(is_end, 1, 2))

    for c in loads[:2]:
        c.wait()

    @pl.when(is_end)
    def _():
        res.wait()

    def rms(v, gain):
        return v * lax.rsqrt(jnp.mean(v * v, axis=-1, keepdims=True) + NORM_EPS) * gain

    def red_copy(stage, recv, s_sem, r_sem, d, slot, i):
        k = lax.rem(i, q)
        return pltpu.make_async_remote_copy(stage.at[slot, d], recv.at[d, k], s_sem.at[slot, d], r_sem.at[d, k],
                                            device_id=toward[d], device_id_type=MESH)

    def cast_copy(s_sem, r_sem, d, i):
        return pltpu.make_async_remote_copy(ub.at[d, i], ub.at[d, i], s_sem.at[d, i], r_sem.at[d, i],
                                            device_id=away[d], device_id_type=MESH)

    def out_copy(d, i):
        return pltpu.make_async_copy(ub.at[d, i], out_hbm.at[pl.ds(pl.multiple_of(d * half + i * C, C), C), :], out_sem.at[d, i])

    def tick(t, _):
        slot = lax.rem(t, 2)

        def free_stage(stage, recv, s_sem, r_sem, first):
            for d in (0, 1):
                i = t - first - 3 + r[d] - 2

                @pl.when((i >= 0) & (i < n) & (r[d] > 0))
                def _():
                    red_copy(stage, recv, s_sem, r_sem, d, slot, i).wait_send()

        def reduce(stage, recv, s_sem, r_sem, first, at_end):
            for d in (0, 1):
                i = t - first - 3 + r[d]
                act = (i >= 0) & (i < n)

                @pl.when(act & (r[d] < 3))
                def _():
                    red_copy(stage, recv, s_sem, r_sem, d, slot, i).wait_recv()
                    stage[slot, d] += recv[d, lax.rem(i, q)]

                @pl.when(act & (r[d] > 0))
                def _():
                    red_copy(stage, recv, s_sem, r_sem, d, slot, i).start()

                @pl.when(act & (r[d] == 0))
                def _():
                    at_end(d, i)

        def spread(s_sem, r_sem, first, then):
            for d in (0, 1):
                i = t - first - r[d]
                act = (i >= 0) & (i < n) & (r[d] > 0)

                @pl.when(act)
                def _():
                    cast_copy(s_sem, r_sem, d, i).wait_recv()

                @pl.when(act & (r[d] < 3))
                def _():
                    cast_copy(s_sem, r_sem, d, i).start()
                if then is not None:
                    @pl.when(act)
                    def _():
                        then(d, i)

        free_stage(so, ro, os_sem, or_sem, 0)

        @pl.when(t < n + 3)
        def _():
            for d in (0, 1):
                i = jnp.clip(t - 3 + r[d], 0, n - 1)
                lhs_a[pl.ds(d * C, C), :] = a_v[pl.ds(pl.multiple_of(d * half + i * C, C), C), :]

            def cols(j, _):
                cs = pl.ds(pl.multiple_of(j * 256, 256), 256)
                p = jnp.dot(lhs_a[...], wo_v[:, cs], preferred_element_type=jnp.float32)
                so[slot, 0, :, cs] = p[:C]
                so[slot, 1, :, cs] = p[C:]
                return 0
            lax.fori_loop(0, D // 256, cols, 0)

        def o_end(d, i):
            rows = pl.ds(pl.multiple_of(i * C, C), C)
            h1 = (hb[rows, :].astype(jnp.float32) + rms(so[slot, d], g_ref[1:2, :])).astype(jnp.bfloat16)
            hb[rows, :] = h1
            ub[d, i] = rms(h1.astype(jnp.float32), g_ref[2:3, :]).astype(jnp.bfloat16)
            cast_copy(us_sem, ur_sem, d, i).start()
        reduce(so, ro, os_sem, or_sem, 0, o_end)
        spread(us_sem, ur_sem, 3, None)

        @pl.when(t == 6)
        def _():
            for c in loads[2:]:
                c.wait()
        free_stage(sm, rm, ms_sem, mr_sem, 6)

        @pl.when((t >= 6) & (t < n + 9))
        def _():
            for d in (0, 1):
                i = t - 9 + r[d]

                @pl.when((i >= 0) & (i < n) & (r[d] < 3))
                def _():
                    cast_copy(us_sem, ur_sem, d, i).wait_send()

                @pl.when((i >= 0) & (i < n))
                def _():
                    lhs_u[pl.ds(d * C, C), :] = ub[d, jnp.clip(i, 0, n - 1)]

            def hidden(cs):
                gate = jnp.dot(lhs_u[...], wg_v[:, cs], preferred_element_type=jnp.float32)
                up = jnp.dot(lhs_u[...], wu_v[:, cs], preferred_element_type=jnp.float32)
                fb[:, cs] = (gate / (1.0 + jnp.exp(-gate)) * up).astype(jnp.bfloat16)

            def hcols(j, _):
                hidden(pl.ds(pl.multiple_of(j * 256, 256), 256))
                return 0
            lax.fori_loop(0, ff // 256, hcols, 0)
            if ff % 256:
                hidden(pl.ds(ff // 256 * 256, ff % 256))

            def dcols(j, _):
                cs = pl.ds(pl.multiple_of(j * 256, 256), 256)
                p = jnp.dot(fb[...], wd_v[:, cs], preferred_element_type=jnp.float32)
                sm[slot, 0, :, cs] = p[:C]
                sm[slot, 1, :, cs] = p[C:]
                return 0
            lax.fori_loop(0, D // 256, dcols, 0)

        def m_end(d, i):
            rows = pl.ds(pl.multiple_of(i * C, C), C)
            ub[d, i] = (hb[rows, :].astype(jnp.float32) + rms(sm[slot, d], g_ref[3:4, :])).astype(jnp.bfloat16)
            cast_copy(hs_sem, hr_sem, d, i).start()
            out_copy(d, i).start()
        reduce(sm, rm, ms_sem, mr_sem, 6, m_end)
        spread(hs_sem, hr_sem, 9, lambda d, i: out_copy(d, i).start())
        return 0

    lax.fori_loop(0, n + 12, tick, 0)

    def drain(i, _):
        for d in (0, 1):
            @pl.when(r[d] < 3)
            def _():
                cast_copy(hs_sem, hr_sem, d, i).wait_send()
            out_copy(d, i).wait()
        return 0
    lax.fori_loop(0, n, drain, 0)


def ffn(layer, a, h, gains, w_o, w_gate, w_up, w_down, C=32, q=4, cid=0):
    t, ka = a.shape
    ff = w_gate.shape[-1]
    n = t // 2 // C
    any_ = pl.BlockSpec(memory_space=pl.ANY)
    bf, f32 = jnp.bfloat16, jnp.float32
    dma = pltpu.SemaphoreType.DMA
    return pl.pallas_call(
        functools.partial(ffn_kernel, layer, C),
        out_shape=jax.ShapeDtypeStruct((t, D), bf),
        in_specs=[any_, any_, pl.BlockSpec(memory_space=pltpu.VMEM), any_, any_, any_, any_],
        out_specs=any_,
        scratch_shapes=[
            pltpu.VMEM((ka, D), bf), pltpu.VMEM((D, ff), bf), pltpu.VMEM((D, ff), bf), pltpu.VMEM((ff, D), bf),
            pltpu.VMEM((t, ka), bf), pltpu.VMEM((t // 2, D), bf), pltpu.VMEM((2, n, C, D), bf),
            pltpu.VMEM((2, 2, C, D), f32), pltpu.VMEM((2, 2, C, D), f32),
            pltpu.VMEM((2, q, C, D), f32), pltpu.VMEM((2, q, C, D), f32),
            pltpu.VMEM((2 * C, ka), bf), pltpu.VMEM((2 * C, D), bf), pltpu.VMEM((2 * C, ff), bf),
            dma((6,)), dma((2, 2)), dma((2, q)), dma((2, 2)), dma((2, q)),
            dma((2, n)), dma((2, n)), dma((2, n)), dma((2, n)), dma((2, n))],
        compiler_params=pltpu.CompilerParams(collective_id=cid, has_side_effects=True, vmem_limit_bytes=67043328),
        cost_estimate=pl.CostEstimate(flops=2 * t * D * (ka + 3 * ff), bytes_accessed=60_000_000, transcendentals=t * ff),
        name=f"ffn{layer}",
    )(a, h, gains, w_o, w_gate, w_up, w_down)


LOCAL_BASE = 10000.0
GLOBAL_BASE = 1000000.0
def tables(pos, base):
    half = 64
    inv_freq = base ** (-jnp.arange(half, dtype=jnp.float32) / half)
    angles = pos.astype(jnp.float32)[:, None] * inv_freq
    c, s = jnp.cos(angles), jnp.sin(angles)
    return jnp.concatenate([c, c], axis=1), jnp.concatenate([-s, s], axis=1)
def solution(mesh):
    def device_fn(x, pos, gains, w_q, w_k, w_v, w_o, w_gate, w_up, w_down):
        h = x
        outs = []
        wo = w_o.reshape(2, 1024, 2560)
        for l in (0, 1):
            local = l == 0
            cos, sin = tables(pos, LOCAL_BASE if local else GLOBAL_BASE)
            wkv = jnp.concatenate([w_k[l].reshape(2560, 256), w_v[l].reshape(2560, 256)], axis=1)
            wq = w_q[l].reshape(2560, 1024)
            a, kc, vc = attn(local, h, gains[l], cos, sin, wkv, wq, cid=l)
            outs += [kc[:, None, :], vc[:, None, :]]
            h = ffn(l, a, h, gains[l], wo, w_gate, w_up, w_down, cid=2 + l)
        return (h, *outs)
    token_spec = P(('rep', 'sp'), None)
    cache_spec = P('rep', ('tp', 'sp'), None)
    in_specs = (token_spec, P(('rep', 'sp')), P(), P(None, None, 'tp', None), P(None, None, 'tp', None),
                P(None, None, 'tp', None), P(None, 'tp', None, None), P(None, None, 'tp'), P(None, None, 'tp'),
                P(None, 'tp', None))
    out_specs = (token_spec, cache_spec, cache_spec, cache_spec, cache_spec)
    return jax.shard_map(device_fn, mesh=mesh, in_specs=in_specs, out_specs=out_specs, check_vma=False)
```

```python
import functools
import jax, jax.numpy as jnp
from jax import lax
from jax.experimental import pallas as pl
from jax.experimental.pallas import tpu as pltpu
from jax.sharding import PartitionSpec as P
MESH = pl.DeviceIdType.MESH
NORM_EPS = 1e-6
D = 2560
WINDOW = 512
HEAD = 128
CHUNK = 32
RING = 4
WD_KEPT = (6, 4)
WD_SLOTS = 2
SPAN = WINDOW + 128
KEYS = 512
LOG2E = 1.4426950408889634
LOCAL_BASE = 10000.0
GLOBAL_BASE = 1000000.0
NT = (((1,), (1,)), ((), ()))
BF, F32 = jnp.bfloat16, jnp.float32


def rms(v, gain):
    return v * lax.rsqrt(jnp.mean(v * v, axis=-1, keepdims=True) + NORM_EPS) * gain


def at(start, size):
    return pl.ds(pl.multiple_of(start, size), size)


def layer_kernel(layer, *refs):
    it = iter(refs)

    def take(k):
        return [next(it) for _ in range(k)]

    if layer == 0:
        x_hbm, g_ref, tab_hbm, wq_hbm, wkv_hbm = take(5)
    else:
        res_hbm, q_hbm, kv_hbm, g_ref = take(4)
    wo_hbm, wg_hbm, wu_hbm, wd_hbm = take(4)
    if layer == 0:
        out_hbm, q1_hbm, kv1_hbm, kc_hbm, vc_hbm = take(5)
    else:
        out_hbm, kc_hbm, vc_hbm = take(3)
    wa, wg_v, wu_v, wd_v, wd_b, q_v, kv, hb, ub, so, sm, ro, rm, lhs_a, lhs_u, fb = take(16)
    w_sem, wo_sem, wk_sem, wd_sem, os_sem, or_sem, ms_sem, mr_sem, us_sem, ur_sem, hs_sem, hr_sem, out_sem, c_sem = take(14)
    if layer == 0:
        tab, wkv_v, uq, qs, ks, cache = take(6)
        (wq_sem, wkv_sem, halo_s, halo_r, tail_s, tail_r, pair_s, pair_r, far_s, far_r, own_s, fwd_s, fwd_r, q_sem) = take(14)
    else:
        st, sc_v = take(2)

    z = lax.axis_index('tp')
    s = lax.axis_index('sp')
    C = CHUNK
    n = hb.shape[0]
    half = n * C
    rows = 2 * half
    ff = wg_v.shape[1]
    scale = HEAD ** -0.5 * LOG2E
    r = (z, 3 - z)
    down = {'tp': jnp.maximum(z - 1, 0)}
    up = {'tp': jnp.minimum(z + 1, 3)}
    toward, away = (down, up), (up, down)
    is_end = (z == 0) | (z == 3)
    pair = {'sp': s + 1 - 2 * lax.rem(s, 2)}
    far_id = lax.rem(s + 2, 4)
    far = {'sp': far_id}

    def load(k, src, dst):
        return pltpu.make_async_copy(src, dst, w_sem.at[k])

    wo_tiles = [pltpu.make_async_copy(wo_hbm.at[layer, :, pl.ds(j * 256, 256)], wa.at[pl.ds(j * 1024, 1024), :], wo_sem.at[j])
                for j in range(D // 256)]
    wg_load = load(0, wg_hbm.at[layer], wg_v)
    wu_load = load(1, wu_hbm.at[layer], wu_v)
    res_half = jnp.where(z == 3, 1, 0)
    if layer == 0:
        res_load = load(2, x_hbm.at[res_half], hb)
        def wkv_loads(l):
            return [pltpu.make_async_copy(wkv_hbm.at[l, h], wkv_v.at[:, pl.ds(h * HEAD, HEAD)], wkv_sem.at[h]) for h in range(4)]
        wq_first = [pltpu.make_async_copy(wq_hbm.at[0, h], wu_v.at[:, pl.ds(h * HEAD, HEAD)], wq_sem.at[h]) for h in range(8)]
        first = [load(3, x_hbm, ub), load(4, tab_hbm.at[0], tab)] + wkv_loads(0) + wq_first
    else:
        res_load = load(2, res_hbm, hb)
        first = [load(3, q_hbm, q_v), load(4, kv_hbm, kv)]
    for c in first:
        c.start()
    for c in wo_tiles:
        c.start()

    @pl.when(is_end)
    def _():
        res_load.start()
    wg_load.start()
    if layer == 1:
        wu_load.start()

    bar = pltpu.get_barrier_semaphore()

    @pl.when(z > 0)
    def _():
        pl.semaphore_signal(bar, inc=1, device_id=down, device_id_type=MESH)

    @pl.when(z < 3)
    def _():
        pl.semaphore_signal(bar, inc=1, device_id=up, device_id_type=MESH)
    if layer == 0:
        for k in (1, 2, 3):
            pl.semaphore_signal(bar, inc=1, device_id={'sp': lax.rem(s + k, 4)}, device_id_type=MESH)
    pl.semaphore_wait(bar, jnp.where(is_end, 1, 2) + (3 if layer == 0 else 0))

    kept = WD_KEPT[layer]
    flow = D // 256 - kept

    def wd_tile(k):
        slot = lax.rem(k, WD_SLOTS)
        return pltpu.make_async_copy(wd_hbm.at[layer, :, at((kept + lax.rem(k, flow)) * 256, 256)], wd_b.at[slot], wd_sem.at[slot])
    wd_total = (n + 3) * flow
    wd_loads = [pltpu.make_async_copy(wd_hbm.at[layer, :, pl.ds(j * 256, 256)], wd_v.at[j], wk_sem.at[j]) for j in range(kept)]

    def rotor(cs):
        low = lax.broadcasted_iota(jnp.int32, cs.shape, 1) < HEAD // 2
        other = pltpu.roll(cs, HEAD // 2, 1)
        cos, sin = jnp.where(low, cs, other), jnp.where(low, -other, cs)
        return lambda v: v * cos + pltpu.roll(v, HEAD // 2, 1) * sin

    if layer == 0:
        kv[:, pl.ds(WINDOW + rows, SPAN - WINDOW), :] = jnp.zeros((4, SPAN - WINDOW, HEAD), BF)

        @pl.when(s == 0)
        def _():
            kv[:, :WINDOW, :] = jnp.zeros((4, WINDOW, HEAD), BF)

        halo = pltpu.make_async_remote_copy(kv.at[:, pl.ds(rows, WINDOW), :], kv.at[:, pl.ds(0, WINDOW), :],
                                            halo_s, halo_r, device_id={'sp': jnp.minimum(s + 1, 3)}, device_id_type=MESH)

        def tail(dst, kind):
            return pltpu.make_async_remote_copy(kv.at[2 * kind + dst // 2, pl.ds(rows, WINDOW), :], cache.at[kind],
                                                tail_s.at[dst, kind], tail_r.at[kind], device_id={'sp': dst}, device_id_type=MESH)
        B = 256
        per = B // C
        blocks = half // B
        for c in first[:6]:
            c.wait()

        def kv_block(k, _):
            d = 1 - k // blocks
            i0 = lax.rem(k, blocks) * per
            row = d * half + i0 * C

            def norm(i, _):
                ub[d, i0 + i] = rms(ub[d, i0 + i].astype(F32), g_ref[0, 0:1, :]).astype(BF)
                return 0
            lax.fori_loop(0, per, norm, 0, unroll=2)
            p = jnp.dot(ub[d, at(i0, per)].reshape(B, D), wkv_v[...], preferred_element_type=F32)
            rope = rotor(tab[at(row, B), :])
            dst = at(WINDOW + row, B)
            for h in range(2):
                kv[h, dst, :] = rope(p[:, h * HEAD:(h + 1) * HEAD]).astype(BF)
                kv[2 + h, dst, :] = p[:, (2 + h) * HEAD:(3 + h) * HEAD].astype(BF)

            @pl.when(k == blocks - 1)
            def _():
                @pl.when(s < 3)
                def _():
                    halo.start()

                @pl.when(s == 3)
                def _():
                    for dst in range(3):
                        for kind in range(2):
                            tail(dst, kind).start()
            return 0
        lax.fori_loop(0, 2 * blocks, kv_block, 0)
        for c in wkv_loads(1):
            c.start()
        for c in wq_first:
            c.wait()

        def q_block(k, _):
            d = k // blocks
            i0 = lax.rem(k, blocks) * per
            rope = rotor(tab[at(d * half + i0 * C, B), :])
            u = ub[d, at(i0, per)].reshape(B, D)
            for c in range(4):
                p = jnp.dot(u, wu_v[:, c * 256:(c + 1) * 256], preferred_element_type=F32)
                for e in range(2):
                    qe = rope(p[:, e * HEAD:(e + 1) * HEAD]).astype(BF)
                    h = (c % 2) * 2 + e
                    for i in range(per):
                        q_v[d, i0 + i, c // 2, h * C:(h + 1) * C, :] = qe[i * C:(i + 1) * C]
            return 0
        lax.fori_loop(0, 2 * blocks, q_block, 0)
        wu_load.start()
        load(4, tab_hbm.at[1], tab).start()

    @pl.when(is_end)
    def _():
        res_load.wait()
    for c in wd_loads:
        c.start()
    for k in range(WD_SLOTS):
        wd_tile(k).start()

    def place(d, g, o):
        for h in range(4):
            lhs_a[d * C:(d + 1) * C, (g * 4 + h) * HEAD:(g * 4 + h + 1) * HEAD] = o[h * C:(h + 1) * C].astype(BF)

    def chunk_at(t, d):
        return jnp.clip(t - 3 + r[d], 0, n - 1)

    def row_col(shape):
        return (lax.rem(lax.broadcasted_iota(jnp.int32, shape, 0), C), lax.broadcasted_iota(jnp.int32, shape, 1))

    def attend_local(t):
        for d in range(2):
            i = chunk_at(t, d)
            keys = pl.ds(pl.multiple_of(d * half + i * C, C), SPAN)
            low = jnp.where(s == 0, WINDOW - d * half - i * C, 0)
            for g in range(2):
                sc = lax.dot_general(q_v[d, i, g], kv[g, keys, :], NT, preferred_element_type=F32) * scale
                row, col = row_col(sc.shape)
                sc = jnp.where((col > row) & (col <= row + WINDOW) & (col >= low), sc, -1e30)
                p = jnp.exp2(sc - jnp.max(sc, axis=1, keepdims=True))
                o = jnp.dot(p.astype(BF), kv[2 + g, keys, :], preferred_element_type=F32)
                place(d, g, o / jnp.sum(p, axis=1, keepdims=True))

    def attend_global(t):
        ids = [chunk_at(t, d) for d in range(2)]
        streams = [(d, g) for d in range(2) for g in range(2)]
        for d, g in streams:
            st[d, g, 0] = jnp.full((4 * C, HEAD), -1e30, F32)
            st[d, g, 1] = jnp.zeros((4 * C, HEAD), F32)
            st[d, g, 2] = jnp.zeros((4 * C, HEAD), F32)

        def score(slot, d, g, b):
            sc_v[slot, d, g] = lax.dot_general(q_v[d, ids[d], g], kv[g, at(b * KEYS, KEYS), :], NT, preferred_element_type=F32)

        def update(slot, d, g, b, masked=False):
            sc = sc_v[slot, d, g]
            if masked:
                row, col = row_col(sc.shape)
                sc = jnp.where(col <= row + ids[d] * C, sc, -1e30)
            old = st[d, g, 0]
            new = jnp.maximum(old, jnp.max(sc, axis=1, keepdims=True))
            alpha = jnp.exp2((old - new) * scale)
            parts = [jnp.exp2((sc[:, c * HEAD:(c + 1) * HEAD] - new) * scale) for c in range(KEYS // HEAD)]
            st[d, g, 1] = st[d, g, 1] * alpha + sum(parts[1:], parts[0])
            p = jnp.concatenate(parts, axis=1).astype(BF)
            st[d, g, 2] = st[d, g, 2] * alpha + jnp.dot(p, kv[2 + g, at(b * KEYS, KEYS), :], preferred_element_type=F32)
            st[d, g, 0] = new

        for d, g in streams:
            score(0, d, g, 0)

        def two(j, _):
            for e in range(2):
                for d, g in streams:
                    score(1 - e, d, g, 2 * j + e + 1)
                for d, g in streams:
                    update(e, d, g, 2 * j + e)
            return 0
        lax.fori_loop(0, s, two, 0)
        for g in range(2):
            score(1, 1, g, 2 * s + 1)
        for d, g in streams:
            update(0, d, g, 2 * s, masked=d == 0)
        for g in range(2):
            update(1, 1, g, 2 * s + 1, masked=True)
        for d, g in streams:
            place(d, g, st[d, g, 2] / jnp.sum(st[d, g, 1], axis=1, keepdims=True))

    if layer == 0:
        @pl.when(s > 0)
        def _():
            halo.wait_recv()
        attend = attend_local
    else:
        for c in first:
            c.wait()
        y = s // 2
        caches = [pltpu.make_async_copy(kv.at[y], kc_hbm, c_sem.at[0]), pltpu.make_async_copy(kv.at[2 + y], vc_hbm, c_sem.at[1])]
        for c in caches:
            c.start()
        attend = attend_global
    attend(0)
    for c in wo_tiles:
        c.wait()

    def red_copy(stage, recv, s_sem, r_sem, d, slot, i):
        k = lax.rem(i, RING)
        return pltpu.make_async_remote_copy(stage.at[slot, d], recv.at[d, k], s_sem.at[slot, d], r_sem.at[d, k],
                                            device_id=toward[d], device_id_type=MESH)

    def cast_copy(s_sem, r_sem, d, i):
        return pltpu.make_async_remote_copy(ub.at[d, i], ub.at[d, i], s_sem.at[d, i], r_sem.at[d, i],
                                            device_id=away[d], device_id_type=MESH)

    def out_copy(d, i):
        return pltpu.make_async_copy(ub.at[d, i], out_hbm.at[i] if layer == 0 else out_hbm.at[d, i], out_sem.at[d, i])

    if layer == 0:
        wq_tiles = [pltpu.make_async_copy(wq_hbm.at[1, h], wa.at[pl.ds(h // 2 * D, D), pl.ds(h % 2 * HEAD, HEAD)], wq_sem.at[h]) for h in range(8)]
        pairs = n // 2

        def span_of(dev, d, k):
            return kv1_hbm.at[:, at(dev * rows + d * half + k * 2 * C, 2 * C), :]

        def kv_own(d, k):
            slot = lax.rem(k, 2)
            return pltpu.make_async_copy(ks.at[slot, d], span_of(s, d, k), own_s.at[slot, d])

        def kv_pair(d, k):
            slot = lax.rem(k, 2)
            return pltpu.make_async_remote_copy(ks.at[slot, d], span_of(s, d, k), pair_s.at[slot, d], pair_r.at[d, k],
                                                device_id=pair, device_id_type=MESH)

        def kv_far(d, k):
            slot = lax.rem(k, 2)
            return pltpu.make_async_remote_copy(ks.at[slot, d], span_of(s, d, k), far_s.at[slot, d], far_r.at[d, k],
                                                device_id=far, device_id_type=MESH)

        def kv_fwd(d, k):
            ref = span_of(far_id, d, k)
            return pltpu.make_async_remote_copy(ref, ref, fwd_s.at[d, k], fwd_r.at[d, k], device_id=pair, device_id_type=MESH)

        def q_out(d, k):
            slot = lax.rem(k, 2)
            return pltpu.make_async_copy(qs.at[slot, d], q1_hbm.at[d, at(2 * k, 2)], q_sem.at[slot, d])

        def sent(k):
            for d in range(2):
                kv_own(d, k).wait()
                kv_pair(d, k).wait_send()
                kv_far(d, k).wait_send()
                q_out(d, k).wait()

        def forward(k):
            for d in range(2):
                kv_far(d, k).wait_recv()
                kv_fwd(d, k).start()

        def next_qkv(k):
            slot = lax.rem(k, 2)

            @pl.when(k >= 2)
            def _():
                sent(k - 2)
            M = 2 * C
            for d in range(2):
                uq[d * M:(d + 1) * M, :] = rms(ub[d, at(2 * k, 2)].reshape(M, D).astype(F32), g_ref[1, 0:1, :]).astype(BF)
            ropes = [rotor(tab[at(d * half + k * M, M), :]) for d in range(2)]
            p = jnp.dot(uq[...], wkv_v[...], preferred_element_type=F32)
            for d in range(2):
                for h in range(2):
                    ks[slot, d, h] = ropes[d](p[d * M:(d + 1) * M, h * HEAD:(h + 1) * HEAD]).astype(BF)
                    ks[slot, d, 2 + h] = p[d * M:(d + 1) * M, (2 + h) * HEAD:(3 + h) * HEAD].astype(BF)
                kv_own(d, k).start()
                kv_pair(d, k).start()
                kv_far(d, k).start()
            for c in range(4):
                p = jnp.dot(uq[...], wa[c * D:(c + 1) * D, :], preferred_element_type=F32)
                for d in range(2):
                    for e in range(2):
                        qe = ropes[d](p[d * M:(d + 1) * M, e * HEAD:(e + 1) * HEAD]).astype(BF)
                        h = (c % 2) * 2 + e
                        for i in range(2):
                            qs[slot, d, i, c // 2, h * C:(h + 1) * C, :] = qe[i * C:(i + 1) * C]
            for d in range(2):
                q_out(d, k).start()

            @pl.when(k >= 1)
            def _():
                forward(k - 1)

    def tick(t, _):
        slot = lax.rem(t, 2)

        def free_stage(stage, recv, s_sem, r_sem, first_tick):
            for d in (0, 1):
                i = t - first_tick - 3 + r[d] - 2

                @pl.when((i >= 0) & (i < n) & (r[d] > 0))
                def _():
                    red_copy(stage, recv, s_sem, r_sem, d, slot, i).wait_send()

        def reduce(stage, recv, s_sem, r_sem, first_tick, at_end):
            for d in (0, 1):
                i = t - first_tick - 3 + r[d]
                act = (i >= 0) & (i < n)

                @pl.when(act & (r[d] < 3))
                def _():
                    red_copy(stage, recv, s_sem, r_sem, d, slot, i).wait_recv()
                    stage[slot, d] += recv[d, lax.rem(i, RING)]

                @pl.when(act & (r[d] > 0))
                def _():
                    red_copy(stage, recv, s_sem, r_sem, d, slot, i).start()

                @pl.when(act & (r[d] == 0))
                def _():
                    at_end(d, i)

        def spread(s_sem, r_sem, first_tick, then):
            for d in (0, 1):
                i = t - first_tick - r[d]
                act = (i >= 0) & (i < n) & (r[d] > 0)

                @pl.when(act)
                def _():
                    cast_copy(s_sem, r_sem, d, i).wait_recv()

                @pl.when(act & (r[d] < 3))
                def _():
                    cast_copy(s_sem, r_sem, d, i).start()
                if then is not None:
                    @pl.when(act)
                    def _():
                        then(d, i)

        free_stage(so, ro, os_sem, or_sem, 0)

        @pl.when(t < n + 3)
        def _():
            def cols(j, _):
                cs = at(j * 256, 256)
                p = jnp.dot(lhs_a[...], wa[at(j * 1024, 1024), :], preferred_element_type=F32)
                so[slot, 0, :, cs] = p[:C]
                so[slot, 1, :, cs] = p[C:]
                return 0
            lax.fori_loop(0, D // 256, cols, 0, unroll=5)

        def o_end(d, i):
            h1 = (hb[i].astype(F32) + rms(so[slot, d], g_ref[layer, 1:2, :])).astype(BF)
            hb[i] = h1
            ub[d, i] = rms(h1.astype(F32), g_ref[layer, 2:3, :]).astype(BF)
            cast_copy(us_sem, ur_sem, d, i).start()
        reduce(so, ro, os_sem, or_sem, 0, o_end)
        spread(us_sem, ur_sem, 3, None)

        @pl.when(t + 1 < n + 3)
        def _():
            attend(t + 1)

        @pl.when(t == 6)
        def _():
            for c in [wg_load, wu_load] + wd_loads:
                c.wait()
        free_stage(sm, rm, ms_sem, mr_sem, 6)

        @pl.when((t >= 6) & (t < n + 9))
        def _():
            for d in (0, 1):
                i = t - 9 + r[d]

                @pl.when((i >= 0) & (i < n) & (r[d] < 3))
                def _():
                    cast_copy(us_sem, ur_sem, d, i).wait_send()

                @pl.when((i >= 0) & (i < n))
                def _():
                    lhs_u[pl.ds(d * C, C), :] = ub[d, jnp.clip(i, 0, n - 1)]

            def hidden(cs):
                gate = jnp.dot(lhs_u[...], wg_v[:, cs], preferred_element_type=F32)
                upper = jnp.dot(lhs_u[...], wu_v[:, cs], preferred_element_type=F32)
                fb[:, cs] = (gate / (1.0 + jnp.exp(-gate)) * upper).astype(BF)

            def hcols(j, _):
                hidden(at(j * 256, 256))
                return 0
            lax.fori_loop(0, ff // 256, hcols, 0, unroll=3)
            if ff % 256:
                hidden(pl.ds(ff // 256 * 256, ff % 256))

            def down_tile(w, j):
                cs = pl.ds(j * 256, 256)
                p = jnp.dot(fb[...], w, preferred_element_type=F32)
                sm[slot, 0, :, cs] = p[:C]
                sm[slot, 1, :, cs] = p[C:]

            def flowing(j):
                k = (t - 6) * flow + j
                wd_tile(k).wait()
                down_tile(wd_b[lax.rem(k, WD_SLOTS)], kept + j)

                @pl.when(k + WD_SLOTS < wd_total)
                def _():
                    wd_tile(k + WD_SLOTS).start()
            for j in range(max(kept, flow)):
                if j < flow:
                    flowing(j)
                if j < kept:
                    down_tile(wd_v[j], j)

        def m_end(d, i):
            ub[d, i] = (hb[i].astype(F32) + rms(sm[slot, d], g_ref[layer, 3:4, :])).astype(BF)
            cast_copy(hs_sem, hr_sem, d, i).start()
            out_copy(d, i).start()
        reduce(sm, rm, ms_sem, mr_sem, 6, m_end)
        spread(hs_sem, hr_sem, 9, None if layer == 0 else lambda d, i: out_copy(d, i).start())

        if layer == 0:
            @pl.when(t == n + 3)
            def _():
                for c in wq_tiles:
                    c.start()
            first_qkv = n + 12 - pairs

            @pl.when(t == first_qkv)
            def _():
                for c in wkv_loads(1) + [load(4, tab_hbm.at[1], tab)] + wq_tiles:
                    c.wait()

            @pl.when(t >= first_qkv)
            def _():
                next_qkv(t - first_qkv)
        return 0

    lax.fori_loop(0, n + 12, tick, 0)

    if layer == 0:
        forward(pairs - 1)

        @pl.when(s < 3)
        def _():
            halo.wait_send()
            for kind in range(2):
                tail(0, kind).wait_recv()

        @pl.when(s == 3)
        def _():
            for dst in range(3):
                for kind in range(2):
                    tail(dst, kind).wait_send()
            for kind in range(2):
                cache[kind] = kv[2 * kind + 1, pl.ds(rows, WINDOW), :]
        caches = [pltpu.make_async_copy(cache.at[0], kc_hbm, c_sem.at[0]), pltpu.make_async_copy(cache.at[1], vc_hbm, c_sem.at[1])]
        for c in caches:
            c.start()
        for k in (pairs - 2, pairs - 1):
            sent(k)

        def got(k, _):
            for d in range(2):
                kv_pair(d, k).wait_recv()
                kv_fwd(d, k).wait()
            return 0
        lax.fori_loop(0, pairs, got, 0)

    def drain(i, _):
        for d in (0, 1):
            @pl.when(r[d] < 3)
            def _():
                cast_copy(hs_sem, hr_sem, d, i).wait_send()
            if layer == 0:
                @pl.when(r[d] == 0)
                def _():
                    out_copy(d, i).wait()
            else:
                out_copy(d, i).wait()
        return 0
    lax.fori_loop(0, n, drain, 0)
    for c in caches:
        c.wait()


def run_layer(layer, heads, weights, out_shape):
    dma = pltpu.SemaphoreType.DMA
    any_, vmem = pl.BlockSpec(memory_space=pl.ANY), pl.BlockSpec(memory_space=pltpu.VMEM)
    ka, ff = weights[0].shape[1], weights[1].shape[2]
    C = CHUNK
    n = out_shape[0].shape[-3]
    rows = 2 * n * C
    keys = WINDOW + rows + SPAN - WINDOW if layer == 0 else 4 * rows
    scratch = [
        pltpu.VMEM((ka * D // 256, 256), BF), pltpu.VMEM((D, ff), BF), pltpu.VMEM((D, ff), BF), pltpu.VMEM((WD_KEPT[layer], ff, 256), BF), pltpu.VMEM((WD_SLOTS, ff, 256), BF),
        pltpu.VMEM((2, n, 2, 4 * C, HEAD), BF), pltpu.VMEM((4, keys, HEAD), BF),
        pltpu.VMEM((n, C, D), BF), pltpu.VMEM((2, n, C, D), BF),
        pltpu.VMEM((2, 2, C, D), F32), pltpu.VMEM((2, 2, C, D), F32),
        pltpu.VMEM((2, RING, C, D), F32), pltpu.VMEM((2, RING, C, D), F32),
        pltpu.VMEM((2 * C, ka), BF), pltpu.VMEM((2 * C, D), BF), pltpu.VMEM((2 * C, ff), BF),
        dma((7,)), dma((D // 256,)), dma((WD_KEPT[layer],)), dma((WD_SLOTS,)), dma((2, 2)), dma((2, RING)), dma((2, 2)), dma((2, RING)),
        dma((2, n)), dma((2, n)), dma((2, n)), dma((2, n)), dma((2, n)), dma((2,))]
    if layer == 0:
        p = n // 2
        scratch += [
            pltpu.VMEM((rows, HEAD), F32), pltpu.VMEM((D, 4 * HEAD), BF), pltpu.VMEM((4 * C, D), BF),
            pltpu.VMEM((2, 2, 2, 2, 4 * C, HEAD), BF), pltpu.VMEM((2, 2, 4, 2 * C, HEAD), BF), pltpu.VMEM((2, WINDOW, HEAD), BF),
            dma((8,)), dma((4,)), dma, dma, dma((3, 2)), dma((2,)), dma((2, 2)), dma((2, p)), dma((2, 2)), dma((2, p)), dma((2, 2)),
            dma((2, p)), dma((2, p)), dma((2, 2))]
        in_specs = [any_, vmem] + [any_] * 3
    else:
        scratch += [pltpu.VMEM((2, 2, 3, 4 * C, HEAD), F32), pltpu.VMEM((2, 2, 2, 4 * C, KEYS), F32)]
        in_specs = [any_, any_, any_, vmem]
    return pl.pallas_call(
        functools.partial(layer_kernel, layer),
        out_shape=out_shape,
        in_specs=in_specs + [any_] * 4,
        out_specs=[any_] * len(out_shape),
        scratch_shapes=scratch,
        compiler_params=pltpu.CompilerParams(collective_id=layer, has_side_effects=True, vmem_limit_bytes=67043328),
        cost_estimate=pl.CostEstimate(flops=2 * rows * D * (ka + 3 * ff), bytes_accessed=300_000_000, transcendentals=rows * ff),
        name=f'layer{layer}',
    )(*heads, *weights)


def solution(mesh):
    def device_fn(x, pos, gains, w_q, w_k, w_v, w_o, w_gate, w_up, w_down):
        C = CHUNK
        rows = x.shape[0]
        n = rows // 2 // C
        shape = jax.ShapeDtypeStruct
        heads_first = (0, 2, 1, 3)
        wq = jnp.transpose(w_q, heads_first)
        wkv = jnp.concatenate([jnp.transpose(w_k, heads_first), jnp.transpose(w_v, heads_first)], axis=1)
        half = HEAD // 2
        freq = jnp.stack([base ** (-jnp.arange(half, dtype=F32) / half) for base in (LOCAL_BASE, GLOBAL_BASE)])
        angles = pos.astype(F32)[None, :, None] * freq[:, None, :]
        tab = jnp.concatenate([jnp.cos(angles), jnp.sin(angles)], axis=2)
        weights = (w_o.reshape(2, 8 * HEAD, D), w_gate, w_up, w_down)
        qshape = shape((2, n, 2, 4 * C, HEAD), BF)
        res, q1, kv1, kl, vl = run_layer(
            0, (x.reshape(2, n, C, D), gains, tab, wq, wkv), weights,
            [shape((n, C, D), BF), qshape, shape((4, 4 * rows, HEAD), BF), shape((WINDOW, HEAD), BF), shape((WINDOW, HEAD), BF)])
        out, kg, vg = run_layer(
            1, (res, q1, kv1, gains), weights,
            [shape((2, n, C, D), BF), shape((4 * rows, HEAD), BF), shape((4 * rows, HEAD), BF)])
        return (out.reshape(rows, D), kl[:, None, :], vl[:, None, :], kg[:, None, :], vg[:, None, :])

    token_spec = P(('rep', 'sp'), None)
    cache_spec = P('rep', ('tp', 'sp'), None)
    in_specs = (token_spec, P(('rep', 'sp')), P(), P(None, None, 'tp', None), P(None, None, 'tp', None),
                P(None, None, 'tp', None), P(None, 'tp', None, None), P(None, None, 'tp'), P(None, None, 'tp'),
                P(None, 'tp', None))
    out_specs = (token_spec, cache_spec, cache_spec, cache_spec, cache_spec)
    return jax.shard_map(device_fn, mesh=mesh, in_specs=in_specs, out_specs=out_specs, check_vma=False)
```

```python
import functools
import jax, jax.numpy as jnp
from jax import lax
from jax.experimental import pallas as pl
from jax.experimental.pallas import tpu as pltpu
from jax.sharding import PartitionSpec as P
MESH = pl.DeviceIdType.MESH
NORM_EPS = 1e-6
D = 2560
WINDOW = 512
HEAD = 128
CHUNK = 32
RING = 4
WD_KEPT = (4, 4)
WD_SLOTS = 2
SPAN = WINDOW + 128
KEYS = 512
LOG2E = 1.4426950408889634
LOCAL_BASE = 10000.0
GLOBAL_BASE = 1000000.0
NT = (((1,), (1,)), ((), ()))
BF, F32 = jnp.bfloat16, jnp.float32


def rms(v, gain):
    return v * lax.rsqrt(jnp.mean(v * v, axis=-1, keepdims=True) + NORM_EPS) * gain


def at(start, size):
    return pl.ds(pl.multiple_of(start, size), size)


def layer_kernel(layer, *refs):
    it = iter(refs)

    def take(k):
        return [next(it) for _ in range(k)]

    if layer == 0:
        x_hbm, g_ref, tab_hbm, wq_hbm, wk_hbm, wv_hbm = take(6)
    else:
        res_hbm, q_hbm, kv_hbm, g_ref = take(4)
    wo_hbm, wg_hbm, wu_hbm, wd_hbm = take(4)
    if layer == 0:
        out_hbm, q1_hbm, kv1_hbm, kc_hbm, vc_hbm, wq1_hbm, wkv1_hbm = take(7)
    else:
        out_hbm, kc_hbm, vc_hbm = take(3)
    wa, wg_v, wu_v, wd_v, wd_b, q_v, kv, hb, ub, so, sm, ro, rm, lhs_a, lhs_u, fb = take(16)
    w_sem, wo_sem, wk_sem, wd_sem, os_sem, or_sem, ms_sem, mr_sem, us_sem, ur_sem, hs_sem, hr_sem, hx_sem, out_sem, c_sem = take(15)
    if layer == 0:
        tab, wkv_v, uq, qs, ks, cache, perm, qin, kvin, qo, kvo = take(11)
        nat_sem, ri_sem, ro_sem = take(3)
        (x_sem, wq_sem, wkv_sem, halo_s, halo_r, tail_s, tail_r, pair_s, pair_r, far_s, far_r, own_s, fwd_s, fwd_r, q_sem) = take(15)
    else:
        st, sc_v = take(2)

    z = lax.axis_index('tp')
    s = lax.axis_index('sp')
    C = CHUNK
    n = hb.shape[0]
    half = n * C
    rows = 2 * half
    ff = wg_v.shape[1]
    scale = HEAD ** -0.5 * LOG2E
    r = (z, 3 - z)
    down = {'tp': jnp.maximum(z - 1, 0)}
    up = {'tp': jnp.minimum(z + 1, 3)}
    toward, away = (down, up), (up, down)
    is_end = (z == 0) | (z == 3)
    pair = {'sp': s + 1 - 2 * lax.rem(s, 2)}
    far_id = lax.rem(s + 2, 4)
    far = {'sp': far_id}

    def load(k, src, dst):
        return pltpu.make_async_copy(src, dst, w_sem.at[k])

    wo_tiles = [pltpu.make_async_copy(wo_hbm.at[layer, :, pl.ds(j * 256, 256)], wa.at[pl.ds(j * 1024, 1024), :], wo_sem.at[j])
                for j in range(D // 256)]
    wg_load = load(0, wg_hbm.at[layer], wg_v)
    wu_load = load(1, wu_hbm.at[layer], wu_v)
    res_half = jnp.where(z == 3, 1, 0)
    if layer == 0:
        res_load = load(2, x_hbm.at[res_half], hb)
        wkv_loads = [pltpu.make_async_copy(wkv1_hbm.at[h], wkv_v.at[:, pl.ds(h * HEAD, HEAD)], wkv_sem.at[h]) for h in range(4)]

        def native(c):
            src = wq_hbm.at[0, pl.ds(c * D, D)] if c < 8 else (wk_hbm if c < 10 else wv_hbm).at[0, pl.ds(c % 2 * D, D)]
            return pltpu.make_async_copy(src, wg_v.at[:, pl.ds(c * HEAD, HEAD)], nat_sem.at[c])
        natives = [native(c) for c in range(12)]
        B = 256
        per = B // C
        blocks = half // B

        def x_load(k):
            part = (1 - k // blocks, pl.ds(k % blocks * per, per))
            return pltpu.make_async_copy(x_hbm.at[part], ub.at[part], x_sem.at[k])
        x_loads = [x_load(k) for k in range(2 * blocks)]
        first = natives[8:] + x_loads[:1] + [load(4, tab_hbm.at[0], tab)] + x_loads[1:] + natives[:8]
    else:
        res_load = load(2, res_hbm, hb)
        first = [load(3, q_hbm, q_v), load(4, kv_hbm, kv)]
    for c in first:
        c.start()
    if layer == 1:
        for c in wo_tiles:
            c.start()

    bar = pltpu.get_barrier_semaphore()

    peers = [{'tp': lax.rem(z + k, 4)} for k in (1, 2, 3)]
    if layer == 0:
        peers += [{'sp': lax.rem(s + k, 4)} for k in (1, 2, 3)]
    for peer in peers:
        pl.semaphore_signal(bar, inc=1, device_id=peer, device_id_type=MESH)
    pl.semaphore_wait(bar, len(peers))

    kept = WD_KEPT[layer]
    flow = D // 256 - kept

    def wd_tile(k):
        slot = lax.rem(k, WD_SLOTS)
        return pltpu.make_async_copy(wd_hbm.at[layer, :, at((kept + lax.rem(k, flow)) * 256, 256)], wd_b.at[slot], wd_sem.at[slot])
    wd_total = (n + 3) * flow
    wd_loads = [pltpu.make_async_copy(wd_hbm.at[layer, :, pl.ds(j * 256, 256)], wd_v.at[j], wk_sem.at[j]) for j in range(kept)]

    def rotor(cs):
        low = lax.broadcasted_iota(jnp.int32, cs.shape, 1) < HEAD // 2
        other = pltpu.roll(cs, HEAD // 2, 1)
        cos, sin = jnp.where(low, cs, other), jnp.where(low, -other, cs)
        return lambda v: v * cos + pltpu.roll(v, HEAD // 2, 1) * sin

    if layer == 0:
        kv[:, pl.ds(WINDOW + rows, SPAN - WINDOW), :] = jnp.zeros((4, SPAN - WINDOW, HEAD), BF)

        @pl.when(s == 0)
        def _():
            kv[:, :WINDOW, :] = jnp.zeros((4, WINDOW, HEAD), BF)

        halo = pltpu.make_async_remote_copy(kv.at[:, pl.ds(rows, WINDOW), :], kv.at[:, pl.ds(0, WINDOW), :],
                                            halo_s, halo_r, device_id={'sp': jnp.minimum(s + 1, 3)}, device_id_type=MESH)

        def tail(dst, kind):
            return pltpu.make_async_remote_copy(kv.at[2 * kind + dst // 2, pl.ds(rows, WINDOW), :], cache.at[kind],
                                                tail_s.at[dst, kind], tail_r.at[kind], device_id={'sp': dst}, device_id_type=MESH)
        for p, group in enumerate((32, 128)):
            row = lax.broadcasted_iota(jnp.int32, (256, 256), 0)
            col = lax.broadcasted_iota(jnp.int32, (256, 256), 1)
            perm[p] = jnp.where(col == lax.rem(row, group) * (256 // group) + row // group, 1.0, 0.0).astype(BF)

        def by_head(p, block):
            return jnp.dot(perm[p], block, preferred_element_type=F32).astype(BF)

        for c in natives[8:]:
            c.wait()

        def sort_kv(k, _):
            for c in range(4):
                w = by_head(1, wg_v[at(k * 256, 256), (8 + c) * HEAD:(9 + c) * HEAD])
                for h in range(2):
                    wkv_v[at(c % 2 * (D // 2) + k * 128, 128), (c // 2 * 2 + h) * HEAD:(c // 2 * 2 + h + 1) * HEAD] = w[h * 128:(h + 1) * 128]
            return 0
        lax.fori_loop(0, D // 256, sort_kv, 0, unroll=2)
        load(4, tab_hbm.at[0], tab).wait()

        def kv_block(k, _):
            d = 1 - k // blocks
            i0 = lax.rem(k, blocks) * per
            row = d * half + i0 * C
            part = ub.at[d, at(i0, per)]
            pltpu.make_async_copy(part, part, x_sem.at[k]).wait()

            def norm(i, _):
                ub[d, i0 + i] = rms(ub[d, i0 + i].astype(F32), g_ref[0, 0:1, :]).astype(BF)
                return 0
            lax.fori_loop(0, per, norm, 0, unroll=2)
            p = jnp.dot(ub[d, at(i0, per)].reshape(B, D), wkv_v[...], preferred_element_type=F32)
            rope = rotor(tab[at(row, B), :])
            dst = at(WINDOW + row, B)
            for h in range(2):
                kv[h, dst, :] = rope(p[:, h * HEAD:(h + 1) * HEAD]).astype(BF)
                kv[2 + h, dst, :] = p[:, (2 + h) * HEAD:(3 + h) * HEAD].astype(BF)

            @pl.when(k == blocks - 1)
            def _():
                @pl.when(s < 3)
                def _():
                    halo.start()

                @pl.when(s == 3)
                def _():
                    for dst in range(3):
                        for kind in range(2):
                            tail(dst, kind).start()
            return 0
        lax.fori_loop(0, 2 * blocks, kv_block, 0)
        for c in natives[:8]:
            c.wait()

        def sort_q(k, _):
            for c in range(8):
                w = by_head(0, wg_v[at(k * 256, 256), c * HEAD:(c + 1) * HEAD])
                for h in range(8):
                    wu_v[at(c * (D // 8) + k * 32, 32), h * HEAD:(h + 1) * HEAD] = w[h * 32:(h + 1) * 32]
            return 0
        lax.fori_loop(0, D // 256, sort_q, 0)
        for c in wo_tiles:
            c.start()

        @pl.when(is_end)
        def _():
            res_load.start()
        wg_load.start()

        def q_block(k, _):
            d = k // blocks
            i0 = lax.rem(k, blocks) * per
            rope = rotor(tab[at(d * half + i0 * C, B), :])
            u = ub[d, at(i0, per)].reshape(B, D)
            for c in range(4):
                p = jnp.dot(u, wu_v[:, c * 256:(c + 1) * 256], preferred_element_type=F32)
                for e in range(2):
                    qe = rope(p[:, e * HEAD:(e + 1) * HEAD]).astype(BF)
                    h = (c % 2) * 2 + e
                    for i in range(per):
                        q_v[d, i0 + i, c // 2, h * C:(h + 1) * C, :] = qe[i * C:(i + 1) * C]
            return 0
        for d in range(2):
            q_block(d * blocks, 0)

    def place(d, g, o):
        for h in range(4):
            lhs_a[d * C:(d + 1) * C, (g * 4 + h) * HEAD:(g * 4 + h + 1) * HEAD] = o[h * C:(h + 1) * C].astype(BF)

    def chunk_at(t, d):
        return jnp.clip(t - 3 + r[d], 0, n - 1)

    def row_col(shape):
        return (lax.rem(lax.broadcasted_iota(jnp.int32, shape, 0), C), lax.broadcasted_iota(jnp.int32, shape, 1))

    def attend_local(t):
        for d in range(2):
            i = chunk_at(t, d)
            keys = pl.ds(pl.multiple_of(d * half + i * C, C), SPAN)
            low = jnp.where(s == 0, WINDOW - d * half - i * C, 0)
            for g in range(2):
                sc = lax.dot_general(q_v[d, i, g], kv[g, keys, :], NT, preferred_element_type=F32) * scale
                row, col = row_col(sc.shape)
                sc = jnp.where((col > row) & (col <= row + WINDOW) & (col >= low), sc, -1e30)
                p = jnp.exp2(sc - jnp.max(sc, axis=1, keepdims=True))
                o = jnp.dot(p.astype(BF), kv[2 + g, keys, :], preferred_element_type=F32)
                place(d, g, o / jnp.sum(p, axis=1, keepdims=True))

    def attend_global(t):
        ids = [chunk_at(t, d) for d in range(2)]
        streams = [(d, g) for d in range(2) for g in range(2)]
        for d, g in streams:
            st[d, g, 0] = jnp.full((4 * C, HEAD), -1e30, F32)
            st[d, g, 1] = jnp.zeros((4 * C, HEAD), F32)
            st[d, g, 2] = jnp.zeros((4 * C, HEAD), F32)

        def score(slot, d, g, b):
            sc_v[slot, d, g] = lax.dot_general(q_v[d, ids[d], g], kv[g, at(b * KEYS, KEYS), :], NT, preferred_element_type=F32)

        def update(slot, d, g, b, masked=False):
            sc = sc_v[slot, d, g]
            if masked:
                row, col = row_col(sc.shape)
                sc = jnp.where(col <= row + ids[d] * C, sc, -1e30)
            old = st[d, g, 0]
            new = jnp.maximum(old, jnp.max(sc, axis=1, keepdims=True))
            alpha = jnp.exp2((old - new) * scale)
            parts = [jnp.exp2((sc[:, c * HEAD:(c + 1) * HEAD] - new) * scale) for c in range(KEYS // HEAD)]
            st[d, g, 1] = st[d, g, 1] * alpha + sum(parts[1:], parts[0])
            p = jnp.concatenate(parts, axis=1).astype(BF)
            st[d, g, 2] = st[d, g, 2] * alpha + jnp.dot(p, kv[2 + g, at(b * KEYS, KEYS), :], preferred_element_type=F32)
            st[d, g, 0] = new

        for d, g in streams:
            score(0, d, g, 0)

        def two(j, _):
            for e in range(2):
                for d, g in streams:
                    score(1 - e, d, g, 2 * j + e + 1)
                for d, g in streams:
                    update(e, d, g, 2 * j + e)
            return 0
        lax.fori_loop(0, s, two, 0)
        for g in range(2):
            score(1, 1, g, 2 * s + 1)
        for d, g in streams:
            update(0, d, g, 2 * s, masked=d == 0)
        for g in range(2):
            update(1, 1, g, 2 * s + 1, masked=True)
        for d, g in streams:
            place(d, g, st[d, g, 2] / jnp.sum(st[d, g, 1], axis=1, keepdims=True))

    if layer == 0:
        @pl.when(s > 0)
        def _():
            halo.wait_recv()
        attend = attend_local
    else:
        for c in first:
            c.wait()

        @pl.when(is_end)
        def _():
            res_load.start()
        wg_load.start()
        wu_load.start()
        y = s // 2
        caches = [pltpu.make_async_copy(kv.at[y], kc_hbm, c_sem.at[0]), pltpu.make_async_copy(kv.at[2 + y], vc_hbm, c_sem.at[1])]
        for c in caches:
            c.start()
        attend = attend_global
    for c in wd_loads:
        c.start()
    for k in range(WD_SLOTS):
        wd_tile(k).start()
    if layer == 0:
        def sort_in(k):
            jobs = [pltpu.make_async_copy(wq_hbm.at[1, at(k * 1280, 1280)], qin, ri_sem.at[0])]
            small = [pltpu.make_async_copy(w.at[1, at(k * 512, 512)], kvin.at[e], ri_sem.at[1 + e]) for e, w in enumerate((wk_hbm, wv_hbm))]
            return jobs, small

        def sort_out(k):
            return (pltpu.make_async_copy(qo, wq1_hbm.at[:, at(k * 160, 160), :], ro_sem.at[0]),
                    pltpu.make_async_copy(kvo, wkv1_hbm.at[:, at(k * 256, 256), :], ro_sem.at[1]))
        q_parts, kv_parts = 8 * D // 1280, 2 * D // 512
        for jobs in sort_in(0):
            for c in jobs:
                c.start()

        def sort_next(t):
            k = t - 1

            @pl.when((k >= 1) & (k <= q_parts))
            def _():
                sort_out(k - 1)[0].wait()

            @pl.when((k >= 1) & (k <= kv_parts))
            def _():
                sort_out(k - 1)[1].wait()

            @pl.when((k >= 0) & (k < q_parts))
            def _():
                sort_in(k)[0][0].wait()
                for e in range(5):
                    w = by_head(0, qin[e * 256:(e + 1) * 256, :])
                    for h in range(8):
                        qo[h, e * 32:(e + 1) * 32, :] = w[h * 32:(h + 1) * 32]
                sort_out(k)[0].start()

                @pl.when(k + 1 < q_parts)
                def _():
                    sort_in(k + 1)[0][0].start()

            @pl.when((k >= 0) & (k < kv_parts))
            def _():
                for c in sort_in(k)[1]:
                    c.wait()
                for e in range(2):
                    for b in range(2):
                        w = by_head(1, kvin[e, b * 256:(b + 1) * 256, :])
                        for h in range(2):
                            kvo[2 * e + h, b * 128:(b + 1) * 128, :] = w[h * 128:(h + 1) * 128]
                sort_out(k)[1].start()

                @pl.when(k + 1 < kv_parts)
                def _():
                    for c in sort_in(k + 1)[1]:
                        c.start()
    attend(0)
    for c in wo_tiles:
        c.wait()

    @pl.when(is_end)
    def _():
        res_load.wait()

    def red_copy(stage, recv, s_sem, r_sem, d, slot, i):
        k = lax.rem(i, RING)
        return pltpu.make_async_remote_copy(stage.at[slot, d], recv.at[d, k], s_sem.at[slot, d], r_sem.at[d, k],
                                            device_id=toward[d], device_id_type=MESH)

    def cast_copy(s_sem, r_sem, d, i):
        return pltpu.make_async_remote_copy(ub.at[d, i], ub.at[d, i], s_sem.at[d, i], r_sem.at[d, i],
                                            device_id=away[d], device_id_type=MESH)

    def last_copy(d, hops):
        i = n - 1
        target = jnp.clip(z + hops if d == 0 else z - hops, 0, 3)
        return pltpu.make_async_remote_copy(ub.at[d, i], ub.at[d, i], hx_sem.at[d, hops - 2], hr_sem.at[d, i],
                                            device_id={'tp': target}, device_id_type=MESH)

    def out_copy(d, i):
        return pltpu.make_async_copy(ub.at[d, i], out_hbm.at[i] if layer == 0 else out_hbm.at[d, i], out_sem.at[d, i])

    if layer == 0:
        wq_tiles = [pltpu.make_async_copy(wq1_hbm.at[h], wa.at[pl.ds(h // 2 * D, D), pl.ds(h % 2 * HEAD, HEAD)], wq_sem.at[h]) for h in range(8)]
        pairs = n // 2

        def span_of(dev, d, k):
            return kv1_hbm.at[:, at(dev * rows + d * half + k * 2 * C, 2 * C), :]

        def kv_own(d, k):
            slot = lax.rem(k, 2)
            return pltpu.make_async_copy(ks.at[slot, d], span_of(s, d, k), own_s.at[slot, d])

        def kv_pair(d, k):
            slot = lax.rem(k, 2)
            return pltpu.make_async_remote_copy(ks.at[slot, d], span_of(s, d, k), pair_s.at[slot, d], pair_r.at[d, k],
                                                device_id=pair, device_id_type=MESH)

        def kv_far(d, k):
            slot = lax.rem(k, 2)
            return pltpu.make_async_remote_copy(ks.at[slot, d], span_of(s, d, k), far_s.at[slot, d], far_r.at[d, k],
                                                device_id=far, device_id_type=MESH)

        def kv_fwd(d, k):
            ref = span_of(far_id, d, k)
            return pltpu.make_async_remote_copy(ref, ref, fwd_s.at[d, k], fwd_r.at[d, k], device_id=pair, device_id_type=MESH)

        def q_out(d, k):
            slot = lax.rem(k, 2)
            return pltpu.make_async_copy(qs.at[slot, d], q1_hbm.at[d, at(2 * k, 2)], q_sem.at[slot, d])

        def sent(k):
            for d in range(2):
                kv_own(d, k).wait()
                kv_pair(d, k).wait_send()
                kv_far(d, k).wait_send()
                q_out(d, k).wait()

        def forward(k):
            for d in range(2):
                kv_far(d, k).wait_recv()
                kv_fwd(d, k).start()

        def next_qkv(k):
            slot = lax.rem(k, 2)

            @pl.when(k >= 2)
            def _():
                sent(k - 2)
            M = 2 * C
            for d in range(2):
                uq[d * M:(d + 1) * M, :] = rms(ub[d, at(2 * k, 2)].reshape(M, D).astype(F32), g_ref[1, 0:1, :]).astype(BF)
            ropes = [rotor(tab[at(d * half + k * M, M), :]) for d in range(2)]
            p = jnp.dot(uq[...], wkv_v[...], preferred_element_type=F32)
            for d in range(2):
                for h in range(2):
                    ks[slot, d, h] = ropes[d](p[d * M:(d + 1) * M, h * HEAD:(h + 1) * HEAD]).astype(BF)
                    ks[slot, d, 2 + h] = p[d * M:(d + 1) * M, (2 + h) * HEAD:(3 + h) * HEAD].astype(BF)
                kv_own(d, k).start()
                kv_pair(d, k).start()
                kv_far(d, k).start()
            for c in range(4):
                p = jnp.dot(uq[...], wa[c * D:(c + 1) * D, :], preferred_element_type=F32)
                for d in range(2):
                    for e in range(2):
                        qe = ropes[d](p[d * M:(d + 1) * M, e * HEAD:(e + 1) * HEAD]).astype(BF)
                        h = (c % 2) * 2 + e
                        for i in range(2):
                            qs[slot, d, i, c // 2, h * C:(h + 1) * C, :] = qe[i * C:(i + 1) * C]
            for d in range(2):
                q_out(d, k).start()

            @pl.when(k >= 1)
            def _():
                forward(k - 1)

    def tick(t, _):
        slot = lax.rem(t, 2)

        def free_stage(stage, recv, s_sem, r_sem, first_tick):
            for d in (0, 1):
                i = t - first_tick - 3 + r[d] - 2

                @pl.when((i >= 0) & (i < n) & (r[d] > 0))
                def _():
                    red_copy(stage, recv, s_sem, r_sem, d, slot, i).wait_send()

        def reduce(stage, recv, s_sem, r_sem, first_tick, at_end):
            for d in (0, 1):
                i = t - first_tick - 3 + r[d]
                act = (i >= 0) & (i < n)

                @pl.when(act & (r[d] < 3))
                def _():
                    red_copy(stage, recv, s_sem, r_sem, d, slot, i).wait_recv()
                    stage[slot, d] += recv[d, lax.rem(i, RING)]

                @pl.when(act & (r[d] > 0))
                def _():
                    red_copy(stage, recv, s_sem, r_sem, d, slot, i).start()

                @pl.when(act & (r[d] == 0))
                def _():
                    at_end(d, i)

        def spread(s_sem, r_sem, first_tick, then, limit=n):
            for d in (0, 1):
                i = t - first_tick - r[d]
                act = (i >= 0) & (i < n) & (r[d] > 0)

                @pl.when(act)
                def _():
                    cast_copy(s_sem, r_sem, d, i).wait_recv()

                @pl.when(act & (r[d] < 3) & (i < limit))
                def _():
                    cast_copy(s_sem, r_sem, d, i).start()
                if then is not None:
                    @pl.when(act)
                    def _():
                        then(d, i)

        free_stage(so, ro, os_sem, or_sem, 0)

        @pl.when(t < n + 3)
        def _():
            def cols(j, _):
                cs = at(j * 256, 256)
                p = jnp.dot(lhs_a[...], wa[at(j * 1024, 1024), :], preferred_element_type=F32)
                so[slot, 0, :, cs] = p[:C]
                so[slot, 1, :, cs] = p[C:]
                return 0
            lax.fori_loop(0, D // 256, cols, 0, unroll=5)

        def o_end(d, i):
            h1 = (hb[i].astype(F32) + rms(so[slot, d], g_ref[layer, 1:2, :])).astype(BF)
            hb[i] = h1
            ub[d, i] = rms(h1.astype(F32), g_ref[layer, 2:3, :]).astype(BF)
            cast_copy(us_sem, ur_sem, d, i).start()
        reduce(so, ro, os_sem, or_sem, 0, o_end)
        spread(us_sem, ur_sem, 3, None)

        @pl.when(t + 1 < n + 3)
        def _():
            attend(t + 1)

        if layer == 0:
            sort_next(t)

            @pl.when(t < 2)
            def _():
                def later(k, _):
                    return q_block(t * blocks + k, 0)
                lax.fori_loop(1, blocks, later, 0)

            @pl.when(t == 1)
            def _():
                wu_load.start()
                load(4, tab_hbm.at[1], tab).start()

        @pl.when(t == 6)
        def _():
            for c in [wg_load, wu_load] + wd_loads:
                c.wait()
        free_stage(sm, rm, ms_sem, mr_sem, 6)

        @pl.when((t >= 6) & (t < n + 9))
        def _():
            for d in (0, 1):
                i = t - 9 + r[d]

                @pl.when((i >= 0) & (i < n) & (r[d] < 3))
                def _():
                    cast_copy(us_sem, ur_sem, d, i).wait_send()

                @pl.when((i >= 0) & (i < n))
                def _():
                    lhs_u[pl.ds(d * C, C), :] = ub[d, jnp.clip(i, 0, n - 1)]

            def hidden(cs):
                gate = jnp.dot(lhs_u[...], wg_v[:, cs], preferred_element_type=F32)
                upper = jnp.dot(lhs_u[...], wu_v[:, cs], preferred_element_type=F32)
                fb[:, cs] = (gate / (1.0 + jnp.exp(-gate)) * upper).astype(BF)

            def hcols(j, _):
                hidden(at(j * 256, 256))
                return 0
            lax.fori_loop(0, ff // 256, hcols, 0, unroll=3)
            if ff % 256:
                hidden(pl.ds(ff // 256 * 256, ff % 256))

            def down_tile(w, j):
                cs = pl.ds(j * 256, 256)
                p = jnp.dot(fb[...], w, preferred_element_type=F32)
                sm[slot, 0, :, cs] = p[:C]
                sm[slot, 1, :, cs] = p[C:]

            def flowing(j):
                k = (t - 6) * flow + j
                wd_tile(k).wait()
                down_tile(wd_b[lax.rem(k, WD_SLOTS)], kept + j)

                @pl.when(k + WD_SLOTS < wd_total)
                def _():
                    wd_tile(k + WD_SLOTS).start()
            for j in range(max(kept, flow)):
                if j < flow:
                    flowing(j)
                if j < kept:
                    down_tile(wd_v[j], j)

        def m_end(d, i):
            ub[d, i] = (hb[i].astype(F32) + rms(sm[slot, d], g_ref[layer, 3:4, :])).astype(BF)
            cast_copy(hs_sem, hr_sem, d, i).start()

            @pl.when(i == n - 1)
            def _():
                for hops in (2, 3):
                    last_copy(d, hops).start()
            out_copy(d, i).start()
        reduce(sm, rm, ms_sem, mr_sem, 6, m_end)
        spread(hs_sem, hr_sem, 9, None if layer == 0 else lambda d, i: out_copy(d, i).start(), n - 1)

        if layer == 0:
            @pl.when(t == n + 3)
            def _():
                for c in wkv_loads + wq_tiles:
                    c.start()
            first_qkv = n + 12 - pairs

            @pl.when(t == first_qkv)
            def _():
                for c in wkv_loads + [load(4, tab_hbm.at[1], tab)] + wq_tiles:
                    c.wait()

            @pl.when(t >= first_qkv)
            def _():
                next_qkv(t - first_qkv)
        return 0

    lax.fori_loop(0, n + 12, tick, 0)

    if layer == 0:
        forward(pairs - 1)

        @pl.when(s < 3)
        def _():
            halo.wait_send()
            for kind in range(2):
                tail(0, kind).wait_recv()

        @pl.when(s == 3)
        def _():
            for dst in range(3):
                for kind in range(2):
                    tail(dst, kind).wait_send()
            for kind in range(2):
                cache[kind] = kv[2 * kind + 1, pl.ds(rows, WINDOW), :]
        caches = [pltpu.make_async_copy(cache.at[0], kc_hbm, c_sem.at[0]), pltpu.make_async_copy(cache.at[1], vc_hbm, c_sem.at[1])]
        for c in caches:
            c.start()
        for k in (pairs - 2, pairs - 1):
            sent(k)

        def got(k, _):
            for d in range(2):
                kv_pair(d, k).wait_recv()
                kv_fwd(d, k).wait()
            return 0
        lax.fori_loop(0, pairs, got, 0)

    def drain(i, _):
        for d in (0, 1):
            @pl.when((r[d] < 3) & ((i < n - 1) | (r[d] == 0)))
            def _():
                cast_copy(hs_sem, hr_sem, d, i).wait_send()

            @pl.when((r[d] == 0) & (i == n - 1))
            def _():
                for hops in (2, 3):
                    last_copy(d, hops).wait_send()
            if layer == 0:
                @pl.when(r[d] == 0)
                def _():
                    out_copy(d, i).wait()
            else:
                out_copy(d, i).wait()
        return 0
    lax.fori_loop(0, n, drain, 0)
    for c in caches:
        c.wait()


def finish_kernel(parts, *refs):
    k = len(parts)
    ins, outs, bufs, sems = refs[:k], refs[k:2 * k], refs[2 * k:3 * k], refs[3 * k:]
    jobs = []
    for p in range(k):
        size = ins[p].shape[0] // parts[p]
        for e in range(parts[p]):
            cut = pl.ds(e * size, size)
            jobs.append((pltpu.make_async_copy(ins[p].at[cut], bufs[p].at[cut], sems[0].at[len(jobs)]),
                         pltpu.make_async_copy(bufs[p].at[cut], outs[p].at[cut], sems[1].at[len(jobs)])))
    for job in jobs:
        job[0].start()
    for job in jobs:
        job[0].wait()
        job[1].start()
    for job in jobs:
        job[1].wait()


def finish(arrays, parts):
    any_ = pl.BlockSpec(memory_space=pl.ANY)
    dma = pltpu.SemaphoreType.DMA
    return pl.pallas_call(
        functools.partial(finish_kernel, parts),
        out_shape=[jax.ShapeDtypeStruct(a.shape, a.dtype) for a in arrays],
        in_specs=[any_] * len(arrays), out_specs=[any_] * len(arrays),
        scratch_shapes=[pltpu.VMEM(a.shape, a.dtype) for a in arrays] + [dma((sum(parts),)), dma((sum(parts),))],
        compiler_params=pltpu.CompilerParams(vmem_limit_bytes=67043328),
        name='finish',
    )(*arrays)


def run_layer(layer, heads, weights, out_shape):
    dma = pltpu.SemaphoreType.DMA
    any_, vmem = pl.BlockSpec(memory_space=pl.ANY), pl.BlockSpec(memory_space=pltpu.VMEM)
    ka, ff = weights[0].shape[1], weights[1].shape[2]
    C = CHUNK
    n = out_shape[0].shape[-3]
    rows = 2 * n * C
    keys = WINDOW + rows + SPAN - WINDOW if layer == 0 else 4 * rows
    scratch = [
        pltpu.VMEM((ka * D // 256, 256), BF), pltpu.VMEM((D, ff), BF), pltpu.VMEM((D, ff), BF), pltpu.VMEM((WD_KEPT[layer], ff, 256), BF), pltpu.VMEM((WD_SLOTS, ff, 256), BF),
        pltpu.VMEM((2, n, 2, 4 * C, HEAD), BF), pltpu.VMEM((4, keys, HEAD), BF),
        pltpu.VMEM((n, C, D), BF), pltpu.VMEM((2, n, C, D), BF),
        pltpu.VMEM((2, 2, C, D), F32), pltpu.VMEM((2, 2, C, D), F32),
        pltpu.VMEM((2, RING, C, D), F32), pltpu.VMEM((2, RING, C, D), F32),
        pltpu.VMEM((2 * C, ka), BF), pltpu.VMEM((2 * C, D), BF), pltpu.VMEM((2 * C, ff), BF),
        dma((7,)), dma((D // 256,)), dma((WD_KEPT[layer],)), dma((WD_SLOTS,)), dma((2, 2)), dma((2, RING)), dma((2, 2)), dma((2, RING)),
        dma((2, n)), dma((2, n)), dma((2, n)), dma((2, n)), dma((2, 2)), dma((2, n)), dma((2,))]
    if layer == 0:
        p = n // 2
        scratch += [
            pltpu.VMEM((rows, HEAD), F32), pltpu.VMEM((D, 4 * HEAD), BF), pltpu.VMEM((4 * C, D), BF),
            pltpu.VMEM((2, 2, 2, 2, 4 * C, HEAD), BF), pltpu.VMEM((2, 2, 4, 2 * C, HEAD), BF), pltpu.VMEM((2, WINDOW, HEAD), BF),
            pltpu.VMEM((2, 256, 256), BF), pltpu.VMEM((1280, HEAD), BF), pltpu.VMEM((2, 512, HEAD), BF),
            pltpu.VMEM((8, 160, HEAD), BF), pltpu.VMEM((4, 256, HEAD), BF), dma((12,)), dma((3,)), dma((2,)),
            dma((rows // 256,)), dma((8,)), dma((4,)), dma, dma, dma((3, 2)), dma((2,)), dma((2, 2)), dma((2, p)), dma((2, 2)), dma((2, p)), dma((2, 2)),
            dma((2, p)), dma((2, p)), dma((2, 2))]
        in_specs = [any_, vmem] + [any_] * 4
    else:
        scratch += [pltpu.VMEM((2, 2, 3, 4 * C, HEAD), F32), pltpu.VMEM((2, 2, 2, 4 * C, KEYS), F32)]
        in_specs = [any_, any_, any_, vmem]
    return pl.pallas_call(
        functools.partial(layer_kernel, layer),
        out_shape=out_shape,
        in_specs=in_specs + [any_] * 4,
        out_specs=[any_] * len(out_shape),
        scratch_shapes=scratch,
        compiler_params=pltpu.CompilerParams(collective_id=layer, has_side_effects=True, vmem_limit_bytes=67043328),
        cost_estimate=pl.CostEstimate(flops=2 * rows * D * (ka + 3 * ff), bytes_accessed=300_000_000, transcendentals=rows * ff),
        name=f'layer{layer}',
    )(*heads, *weights)


def solution(mesh):
    def device_fn(x, pos, gains, w_q, w_k, w_v, w_o, w_gate, w_up, w_down):
        C = CHUNK
        rows = x.shape[0]
        n = rows // 2 // C
        shape = jax.ShapeDtypeStruct
        wq, wk, wv = (w.reshape(2, -1, HEAD) for w in (w_q, w_k, w_v))
        half = HEAD // 2
        freq = jnp.stack([base ** (-jnp.arange(half, dtype=F32) / half) for base in (LOCAL_BASE, GLOBAL_BASE)])
        grain = 32
        coarse = pos.astype(F32)[::grain][None, :, None] * freq[:, None, :]
        fine = jnp.arange(grain, dtype=F32)[None, :, None] * freq[:, None, :]
        ca, sa, cb, sb = lax.optimization_barrier((jnp.cos(coarse), jnp.sin(coarse), jnp.cos(fine), jnp.sin(fine)))
        ca, sa, cb, sb = ca[:, :, None], sa[:, :, None], cb[:, None], sb[:, None]
        tab = jnp.concatenate([ca * cb - sa * sb, sa * cb + ca * sb], axis=3).reshape(2, rows, HEAD)
        weights = (w_o.reshape(2, 8 * HEAD, D), w_gate, w_up, w_down)
        qshape = shape((2, n, 2, 4 * C, HEAD), BF)
        res, q1, kv1, kl, vl, _, _ = run_layer(
            0, (x.reshape(2, n, C, D), gains, tab, wq, wk, wv), weights,
            [shape((n, C, D), BF), qshape, shape((4, 4 * rows, HEAD), BF), shape((WINDOW, HEAD), BF), shape((WINDOW, HEAD), BF),
             shape((8, D, HEAD), BF), shape((4, D, HEAD), BF)])
        out, kg, vg = run_layer(
            1, (res, q1, kv1, gains), weights,
            [shape((2, n, C, D), BF), shape((4 * rows, HEAD), BF), shape((4 * rows, HEAD), BF)])
        out, kl, vl, kg, vg = finish((out.reshape(rows, D), kl, vl, kg, vg), (8, 1, 1, 2, 2))
        return (out, kl[:, None, :], vl[:, None, :], kg[:, None, :], vg[:, None, :])

    token_spec = P(('rep', 'sp'), None)
    cache_spec = P('rep', ('tp', 'sp'), None)
    in_specs = (token_spec, P(('rep', 'sp')), P(), P(None, None, 'tp', None), P(None, None, 'tp', None),
                P(None, None, 'tp', None), P(None, 'tp', None, None), P(None, None, 'tp'), P(None, None, 'tp'),
                P(None, 'tp', None))
    out_specs = (token_spec, cache_spec, cache_spec, cache_spec, cache_spec)
    return jax.shard_map(device_fn, mesh=mesh, in_specs=in_specs, out_specs=out_specs, check_vma=False)
```

```python
import functools
import jax, jax.numpy as jnp
from jax import lax
from jax.experimental import pallas as pl
from jax.experimental.pallas import tpu as pltpu
from jax.sharding import PartitionSpec as P
MESH = pl.DeviceIdType.MESH
NORM_EPS = 1e-6
D = 2560
WINDOW = 512
HEAD = 128
CHUNK = 32
RING = 4
WD_KEPT = (4, 4)
WD_SLOTS = 2
SPAN = WINDOW + 128
KEYS = 512
LOG2E = 1.4426950408889634
LOCAL_BASE = 10000.0
GLOBAL_BASE = 1000000.0
NT = (((1,), (1,)), ((), ()))
BF, F32 = jnp.bfloat16, jnp.float32


def rms(v, gain):
    return v * lax.rsqrt(jnp.mean(v * v, axis=-1, keepdims=True) + NORM_EPS) * gain


def at(start, size):
    return pl.ds(pl.multiple_of(start, size), size)


def layer_kernel(layer, *refs):
    it = iter(refs)

    def take(k):
        return [next(it) for _ in range(k)]

    if layer == 0:
        x_hbm, g_ref, tab_hbm, wq_hbm, wk_hbm, wv_hbm = take(6)
    else:
        res_hbm, q_hbm, kv_hbm, g_ref = take(4)
    wo_hbm, wg_hbm, wu_hbm, wd_hbm = take(4)
    if layer == 0:
        out_hbm, q1_hbm, kv1_hbm, kc_hbm, vc_hbm, wq1_hbm, wkv1_hbm = take(7)
    else:
        out_hbm, kc_hbm, vc_hbm = take(3)
    wa, wg_v, wu_v, wd_v, wd_b, q_v, kv, hb, ub, so, sm, ro, rm, lhs_a, lhs_u, fb = take(16)
    w_sem, wo_sem, wk_sem, wd_sem, os_sem, or_sem, ms_sem, mr_sem, us_sem, ur_sem, hs_sem, hr_sem, hx_sem, out_sem, c_sem = take(15)
    if layer == 0:
        tab, wkv_v, uq, qs, ks, cache, perm, qin, kvin, qo, kvo = take(11)
        nat_sem, ri_sem, ro_sem = take(3)
        (x_sem, wq_sem, wkv_sem, halo_s, halo_r, tail_s, tail_r, pair_s, pair_r, far_s, far_r, own_s, fwd_s, fwd_r, q_sem) = take(15)
    else:
        st, sc_v = take(2)

    z = lax.axis_index('tp')
    s = lax.axis_index('sp')
    C = CHUNK
    n = hb.shape[0]
    half = n * C
    rows = 2 * half
    ff = wg_v.shape[1]
    scale = HEAD ** -0.5 * LOG2E
    r = (z, 3 - z)
    down = {'tp': jnp.maximum(z - 1, 0)}
    up = {'tp': jnp.minimum(z + 1, 3)}
    toward, away = (down, up), (up, down)
    is_end = (z == 0) | (z == 3)
    pair = {'sp': s + 1 - 2 * lax.rem(s, 2)}
    far_id = lax.rem(s + 2, 4)
    far = {'sp': far_id}

    def load(k, src, dst):
        return pltpu.make_async_copy(src, dst, w_sem.at[k])

    wo_tiles = [pltpu.make_async_copy(wo_hbm.at[layer, :, pl.ds(j * 256, 256)], wa.at[pl.ds(j * 1024, 1024), :], wo_sem.at[j])
                for j in range(D // 256)]
    wg_load = load(0, wg_hbm.at[layer], wg_v)
    wu_load = load(1, wu_hbm.at[layer], wu_v)
    res_half = jnp.where(z == 3, 1, 0)
    if layer == 0:
        res_load = load(2, x_hbm.at[res_half], hb)
        wkv_loads = [pltpu.make_async_copy(wkv1_hbm.at[h], wkv_v.at[:, pl.ds(h * HEAD, HEAD)], wkv_sem.at[h]) for h in range(4)]

        def native(c):
            src = wq_hbm.at[0, pl.ds(c * D, D)] if c < 8 else (wk_hbm if c < 10 else wv_hbm).at[0, pl.ds(c % 2 * D, D)]
            return pltpu.make_async_copy(src, wg_v.at[:, pl.ds(c * HEAD, HEAD)], nat_sem.at[c])
        natives = [native(c) for c in range(12)]
        B = 256
        per = B // C
        blocks = half // B

        def x_load(k):
            part = (1 - k // blocks, pl.ds(k % blocks * per, per))
            return pltpu.make_async_copy(x_hbm.at[part], ub.at[part], x_sem.at[k])
        x_loads = [x_load(k) for k in range(2 * blocks)]
        first = natives[8:] + x_loads[:1] + [load(4, tab_hbm.at[0], tab)] + x_loads[1:] + natives[:8]
    else:
        res_load = load(2, res_hbm, hb)
        first = [load(3, q_hbm, q_v), load(4, kv_hbm, kv)]
    for c in first:
        c.start()
    if layer == 1:
        for c in wo_tiles:
            c.start()

    bar = pltpu.get_barrier_semaphore()

    peers = [{'tp': lax.rem(z + k, 4)} for k in (1, 2, 3)]
    if layer == 0:
        peers += [{'sp': lax.rem(s + k, 4)} for k in (1, 2, 3)]
    for peer in peers:
        pl.semaphore_signal(bar, inc=1, device_id=peer, device_id_type=MESH)
    pl.semaphore_wait(bar, len(peers))

    kept = WD_KEPT[layer]
    flow = D // 256 - kept

    def wd_tile(k):
        slot = lax.rem(k, WD_SLOTS)
        return pltpu.make_async_copy(wd_hbm.at[layer, :, at((kept + lax.rem(k, flow)) * 256, 256)], wd_b.at[slot], wd_sem.at[slot])
    wd_total = (n + 3) * flow
    wd_loads = [pltpu.make_async_copy(wd_hbm.at[layer, :, pl.ds(j * 256, 256)], wd_v.at[j], wk_sem.at[j]) for j in range(kept)]

    def rotor(cs):
        low = lax.broadcasted_iota(jnp.int32, cs.shape, 1) < HEAD // 2
        other = pltpu.roll(cs, HEAD // 2, 1)
        cos, sin = jnp.where(low, cs, other), jnp.where(low, -other, cs)
        return lambda v: v * cos + pltpu.roll(v, HEAD // 2, 1) * sin

    if layer == 0:
        kv[:, pl.ds(WINDOW + rows, SPAN - WINDOW), :] = jnp.zeros((4, SPAN - WINDOW, HEAD), BF)

        @pl.when(s == 0)
        def _():
            kv[:, :WINDOW, :] = jnp.zeros((4, WINDOW, HEAD), BF)

        halo = pltpu.make_async_remote_copy(kv.at[:, pl.ds(rows, WINDOW), :], kv.at[:, pl.ds(0, WINDOW), :],
                                            halo_s, halo_r, device_id={'sp': jnp.minimum(s + 1, 3)}, device_id_type=MESH)

        def tail(dst, kind):
            return pltpu.make_async_remote_copy(kv.at[2 * kind + dst // 2, pl.ds(rows, WINDOW), :], cache.at[kind],
                                                tail_s.at[dst, kind], tail_r.at[kind], device_id={'sp': dst}, device_id_type=MESH)
        for p, group in enumerate((32, 128)):
            row = lax.broadcasted_iota(jnp.int32, (256, 256), 0)
            col = lax.broadcasted_iota(jnp.int32, (256, 256), 1)
            perm[p] = jnp.where(col == lax.rem(row, group) * (256 // group) + row // group, 1.0, 0.0).astype(BF)

        def by_head(p, block):
            return jnp.dot(perm[p], block, preferred_element_type=F32).astype(BF)

        for c in natives[8:]:
            c.wait()

        def sort_kv(k, _):
            for c in range(4):
                w = by_head(1, wg_v[at(k * 256, 256), (8 + c) * HEAD:(9 + c) * HEAD])
                for h in range(2):
                    wkv_v[at(c % 2 * (D // 2) + k * 128, 128), (c // 2 * 2 + h) * HEAD:(c // 2 * 2 + h + 1) * HEAD] = w[h * 128:(h + 1) * 128]
            return 0
        lax.fori_loop(0, D // 256, sort_kv, 0, unroll=5)
        load(4, tab_hbm.at[0], tab).wait()

        def kv_block(k, _):
            d = 1 - k // blocks
            i0 = lax.rem(k, blocks) * per
            row = d * half + i0 * C
            part = ub.at[d, at(i0, per)]
            pltpu.make_async_copy(part, part, x_sem.at[k]).wait()

            def norm(i, _):
                ub[d, i0 + i] = rms(ub[d, i0 + i].astype(F32), g_ref[0, 0:1, :]).astype(BF)
                return 0
            lax.fori_loop(0, per, norm, 0, unroll=4)
            p = jnp.dot(ub[d, at(i0, per)].reshape(B, D), wkv_v[...], preferred_element_type=F32)
            rope = rotor(tab[at(row, B), :])
            dst = at(WINDOW + row, B)
            for h in range(2):
                kv[h, dst, :] = rope(p[:, h * HEAD:(h + 1) * HEAD]).astype(BF)
                kv[2 + h, dst, :] = p[:, (2 + h) * HEAD:(3 + h) * HEAD].astype(BF)

            @pl.when(k == blocks - 1)
            def _():
                @pl.when(s < 3)
                def _():
                    halo.start()

                @pl.when(s == 3)
                def _():
                    for dst in range(3):
                        for kind in range(2):
                            tail(dst, kind).start()
            return 0
        lax.fori_loop(0, 2 * blocks, kv_block, 0)
        for c in natives[:8]:
            c.wait()

        def sort_q(k, _):
            for c in range(8):
                w = by_head(0, wg_v[at(k * 256, 256), c * HEAD:(c + 1) * HEAD])
                for h in range(8):
                    wu_v[at(c * (D // 8) + k * 32, 32), h * HEAD:(h + 1) * HEAD] = w[h * 32:(h + 1) * 32]
            return 0
        lax.fori_loop(0, D // 256, sort_q, 0)
        for c in wo_tiles:
            c.start()

        @pl.when(is_end)
        def _():
            res_load.start()
        wg_load.start()

        def q_block(k, _):
            d = k // blocks
            i0 = lax.rem(k, blocks) * per
            rope = rotor(tab[at(d * half + i0 * C, B), :])
            u = ub[d, at(i0, per)].reshape(B, D)
            for c in range(4):
                p = jnp.dot(u, wu_v[:, c * 256:(c + 1) * 256], preferred_element_type=F32)
                for e in range(2):
                    qe = rope(p[:, e * HEAD:(e + 1) * HEAD]).astype(BF)
                    h = (c % 2) * 2 + e
                    for i in range(per):
                        q_v[d, i0 + i, c // 2, h * C:(h + 1) * C, :] = qe[i * C:(i + 1) * C]
            return 0
        for d in range(2):
            q_block(d * blocks, 0)

    def place(d, g, o):
        for h in range(4):
            lhs_a[d * C:(d + 1) * C, (g * 4 + h) * HEAD:(g * 4 + h + 1) * HEAD] = o[h * C:(h + 1) * C].astype(BF)

    def chunk_at(t, d):
        return jnp.clip(t - 3 + r[d], 0, n - 1)

    def row_col(shape):
        return (lax.rem(lax.broadcasted_iota(jnp.int32, shape, 0), C), lax.broadcasted_iota(jnp.int32, shape, 1))

    def attend_local(t):
        for d in range(2):
            i = chunk_at(t, d)
            keys = pl.ds(pl.multiple_of(d * half + i * C, C), SPAN)
            low = jnp.where(s == 0, WINDOW - d * half - i * C, 0)
            for g in range(2):
                sc = lax.dot_general(q_v[d, i, g], kv[g, keys, :], NT, preferred_element_type=F32) * scale
                row, col = row_col(sc.shape)
                sc = jnp.where((col > row) & (col <= row + WINDOW) & (col >= low), sc, -1e30)
                p = jnp.exp2(sc - jnp.max(sc, axis=1, keepdims=True))
                o = jnp.dot(p.astype(BF), kv[2 + g, keys, :], preferred_element_type=F32)
                place(d, g, o / jnp.sum(p, axis=1, keepdims=True))

    def attend_global(t):
        here = [(t - 3 + r[d] >= 0) & (t - 3 + r[d] < n) for d in range(2)]
        both = here[0] & here[1]
        for halves, cond in (((0, 1), both), ((0,), here[0] & ~both), ((1,), here[1] & ~both)):
            @pl.when(cond)
            def _():
                attend_halves(t, halves)

    def attend_halves(t, halves):
        ids = [chunk_at(t, d) for d in range(2)]
        streams = [(d, g) for d in halves for g in range(2)]
        for d, g in streams:
            st[d, g, 0] = jnp.full((4 * C, HEAD), -1e30, F32)
            st[d, g, 1] = jnp.zeros((4 * C, HEAD), F32)
            st[d, g, 2] = jnp.zeros((4 * C, HEAD), F32)

        def score(slot, d, g, b):
            sc_v[slot, d, g] = lax.dot_general(q_v[d, ids[d], g], kv[g, at(b * KEYS, KEYS), :], NT, preferred_element_type=F32)

        def update(slot, d, g, b, masked=False):
            sc = sc_v[slot, d, g]
            if masked:
                row, col = row_col(sc.shape)
                sc = jnp.where(col <= row + ids[d] * C, sc, -1e30)
            old = st[d, g, 0]
            new = jnp.maximum(old, jnp.max(sc, axis=1, keepdims=True))
            alpha = jnp.exp2((old - new) * scale)
            parts = [jnp.exp2((sc[:, c * HEAD:(c + 1) * HEAD] - new) * scale) for c in range(KEYS // HEAD)]
            st[d, g, 1] = st[d, g, 1] * alpha + sum(parts[1:], parts[0])
            p = jnp.concatenate(parts, axis=1).astype(BF)
            st[d, g, 2] = st[d, g, 2] * alpha + jnp.dot(p, kv[2 + g, at(b * KEYS, KEYS), :], preferred_element_type=F32)
            st[d, g, 0] = new

        for d, g in streams:
            score(0, d, g, 0)

        def two(j, _):
            for e in range(2):
                for d, g in streams:
                    score(1 - e, d, g, 2 * j + e + 1)
                for d, g in streams:
                    update(e, d, g, 2 * j + e)
            return 0
        lax.fori_loop(0, s, two, 0)
        late = [(d, g) for d, g in streams if d == 1]
        for d, g in late:
            score(1, d, g, 2 * s + 1)
        for d, g in streams:
            update(0, d, g, 2 * s, masked=d == 0)
        for d, g in late:
            update(1, d, g, 2 * s + 1, masked=True)
        for d, g in streams:
            place(d, g, st[d, g, 2] / jnp.sum(st[d, g, 1], axis=1, keepdims=True))

    if layer == 0:
        @pl.when(s > 0)
        def _():
            halo.wait_recv()
        attend = attend_local
    else:
        for c in first:
            c.wait()

        @pl.when(is_end)
        def _():
            res_load.start()
        wg_load.start()
        wu_load.start()
        y = s // 2
        caches = [pltpu.make_async_copy(kv.at[y], kc_hbm, c_sem.at[0]), pltpu.make_async_copy(kv.at[2 + y], vc_hbm, c_sem.at[1])]
        for c in caches:
            c.start()
        lhs_a[...] = jnp.zeros_like(lhs_a)
        attend = attend_global
    for c in wd_loads:
        c.start()
    for k in range(WD_SLOTS):
        wd_tile(k).start()
    if layer == 0:
        def sort_in(k):
            jobs = [pltpu.make_async_copy(wq_hbm.at[1, at(k * 1280, 1280)], qin, ri_sem.at[0])]
            small = [pltpu.make_async_copy(w.at[1, at(k * 512, 512)], kvin.at[e], ri_sem.at[1 + e]) for e, w in enumerate((wk_hbm, wv_hbm))]
            return jobs, small

        def sort_out(k):
            return (pltpu.make_async_copy(qo, wq1_hbm.at[:, at(k * 160, 160), :], ro_sem.at[0]),
                    pltpu.make_async_copy(kvo, wkv1_hbm.at[:, at(k * 256, 256), :], ro_sem.at[1]))
        q_parts, kv_parts = 8 * D // 1280, 2 * D // 512
        for jobs in sort_in(0):
            for c in jobs:
                c.start()

        def sort_next(t):
            k = t - 1

            @pl.when((k >= 1) & (k <= q_parts))
            def _():
                sort_out(k - 1)[0].wait()

            @pl.when((k >= 1) & (k <= kv_parts))
            def _():
                sort_out(k - 1)[1].wait()

            @pl.when((k >= 0) & (k < q_parts))
            def _():
                sort_in(k)[0][0].wait()
                for e in range(5):
                    w = by_head(0, qin[e * 256:(e + 1) * 256, :])
                    for h in range(8):
                        qo[h, e * 32:(e + 1) * 32, :] = w[h * 32:(h + 1) * 32]
                sort_out(k)[0].start()

                @pl.when(k + 1 < q_parts)
                def _():
                    sort_in(k + 1)[0][0].start()

            @pl.when((k >= 0) & (k < kv_parts))
            def _():
                for c in sort_in(k)[1]:
                    c.wait()
                for e in range(2):
                    for b in range(2):
                        w = by_head(1, kvin[e, b * 256:(b + 1) * 256, :])
                        for h in range(2):
                            kvo[2 * e + h, b * 128:(b + 1) * 128, :] = w[h * 128:(h + 1) * 128]
                sort_out(k)[1].start()

                @pl.when(k + 1 < kv_parts)
                def _():
                    for c in sort_in(k + 1)[1]:
                        c.start()
    attend(0)
    for c in wo_tiles:
        c.wait()

    @pl.when(is_end)
    def _():
        res_load.wait()

    def red_copy(stage, recv, s_sem, r_sem, d, slot, i):
        k = lax.rem(i, RING)
        return pltpu.make_async_remote_copy(stage.at[slot, d], recv.at[d, k], s_sem.at[slot, d], r_sem.at[d, k],
                                            device_id=toward[d], device_id_type=MESH)

    def cast_copy(s_sem, r_sem, d, i):
        return pltpu.make_async_remote_copy(ub.at[d, i], ub.at[d, i], s_sem.at[d, i], r_sem.at[d, i],
                                            device_id=away[d], device_id_type=MESH)

    def last_copy(d, hops):
        i = n - 1
        target = jnp.clip(z + hops if d == 0 else z - hops, 0, 3)
        return pltpu.make_async_remote_copy(ub.at[d, i], ub.at[d, i], hx_sem.at[d, hops - 2], hr_sem.at[d, i],
                                            device_id={'tp': target}, device_id_type=MESH)

    def out_copy(d, i):
        return pltpu.make_async_copy(ub.at[d, i], out_hbm.at[i] if layer == 0 else out_hbm.at[d, i], out_sem.at[d, i])

    if layer == 0:
        wq_tiles = [pltpu.make_async_copy(wq1_hbm.at[h], wa.at[pl.ds(h // 2 * D, D), pl.ds(h % 2 * HEAD, HEAD)], wq_sem.at[h]) for h in range(8)]
        pairs = n // 2

        def span_of(dev, d, k):
            return kv1_hbm.at[:, at(dev * rows + d * half + k * 2 * C, 2 * C), :]

        def kv_own(d, k):
            slot = lax.rem(k, 2)
            return pltpu.make_async_copy(ks.at[slot, d], span_of(s, d, k), own_s.at[slot, d])

        def kv_pair(d, k):
            slot = lax.rem(k, 2)
            return pltpu.make_async_remote_copy(ks.at[slot, d], span_of(s, d, k), pair_s.at[slot, d], pair_r.at[d, k],
                                                device_id=pair, device_id_type=MESH)

        def kv_far(d, k):
            slot = lax.rem(k, 2)
            return pltpu.make_async_remote_copy(ks.at[slot, d], span_of(s, d, k), far_s.at[slot, d], far_r.at[d, k],
                                                device_id=far, device_id_type=MESH)

        def kv_fwd(d, k):
            ref = span_of(far_id, d, k)
            return pltpu.make_async_remote_copy(ref, ref, fwd_s.at[d, k], fwd_r.at[d, k], device_id=pair, device_id_type=MESH)

        def q_out(d, k):
            slot = lax.rem(k, 2)
            return pltpu.make_async_copy(qs.at[slot, d], q1_hbm.at[d, at(2 * k, 2)], q_sem.at[slot, d])

        def sent(k):
            for d in range(2):
                kv_own(d, k).wait()
                kv_pair(d, k).wait_send()
                kv_far(d, k).wait_send()
                q_out(d, k).wait()

        def forward(k):
            for d in range(2):
                kv_far(d, k).wait_recv()
                kv_fwd(d, k).start()

        def next_qkv(k):
            slot = lax.rem(k, 2)

            @pl.when(k >= 2)
            def _():
                sent(k - 2)
            M = 2 * C
            for d in range(2):
                uq[d * M:(d + 1) * M, :] = rms(ub[d, at(2 * k, 2)].reshape(M, D).astype(F32), g_ref[1, 0:1, :]).astype(BF)
            ropes = [rotor(tab[at(d * half + k * M, M), :]) for d in range(2)]
            p = jnp.dot(uq[...], wkv_v[...], preferred_element_type=F32)
            for d in range(2):
                for h in range(2):
                    ks[slot, d, h] = ropes[d](p[d * M:(d + 1) * M, h * HEAD:(h + 1) * HEAD]).astype(BF)
                    ks[slot, d, 2 + h] = p[d * M:(d + 1) * M, (2 + h) * HEAD:(3 + h) * HEAD].astype(BF)
                kv_own(d, k).start()
                kv_pair(d, k).start()
                kv_far(d, k).start()
            for c in range(4):
                p = jnp.dot(uq[...], wa[c * D:(c + 1) * D, :], preferred_element_type=F32)
                for d in range(2):
                    for e in range(2):
                        qe = ropes[d](p[d * M:(d + 1) * M, e * HEAD:(e + 1) * HEAD]).astype(BF)
                        h = (c % 2) * 2 + e
                        for i in range(2):
                            qs[slot, d, i, c // 2, h * C:(h + 1) * C, :] = qe[i * C:(i + 1) * C]
            for d in range(2):
                q_out(d, k).start()

            @pl.when(k >= 1)
            def _():
                forward(k - 1)

    def tick(t, _):
        slot = lax.rem(t, 2)

        def free_stage(stage, recv, s_sem, r_sem, first_tick):
            for d in (0, 1):
                i = t - first_tick - 3 + r[d] - 2

                @pl.when((i >= 0) & (i < n) & (r[d] > 0))
                def _():
                    red_copy(stage, recv, s_sem, r_sem, d, slot, i).wait_send()

        def reduce(stage, recv, s_sem, r_sem, first_tick, at_end):
            for d in (0, 1):
                i = t - first_tick - 3 + r[d]
                act = (i >= 0) & (i < n)

                @pl.when(act & (r[d] < 3))
                def _():
                    red_copy(stage, recv, s_sem, r_sem, d, slot, i).wait_recv()
                    stage[slot, d] += recv[d, lax.rem(i, RING)]

                @pl.when(act & (r[d] > 0))
                def _():
                    red_copy(stage, recv, s_sem, r_sem, d, slot, i).start()

                @pl.when(act & (r[d] == 0))
                def _():
                    at_end(d, i)

        def spread(s_sem, r_sem, first_tick, then, limit=n):
            for d in (0, 1):
                i = t - first_tick - r[d]
                act = (i >= 0) & (i < n) & (r[d] > 0)

                @pl.when(act)
                def _():
                    cast_copy(s_sem, r_sem, d, i).wait_recv()

                @pl.when(act & (r[d] < 3) & (i < limit))
                def _():
                    cast_copy(s_sem, r_sem, d, i).start()
                if then is not None:
                    @pl.when(act)
                    def _():
                        then(d, i)

        free_stage(so, ro, os_sem, or_sem, 0)

        @pl.when(t < n + 3)
        def _():
            def cols(j, _):
                cs = at(j * 256, 256)
                p = jnp.dot(lhs_a[...], wa[at(j * 1024, 1024), :], preferred_element_type=F32)
                so[slot, 0, :, cs] = p[:C]
                so[slot, 1, :, cs] = p[C:]
                return 0
            lax.fori_loop(0, D // 256, cols, 0, unroll=5)

        def o_end(d, i):
            h1 = (hb[i].astype(F32) + rms(so[slot, d], g_ref[layer, 1:2, :])).astype(BF)
            hb[i] = h1
            ub[d, i] = rms(h1.astype(F32), g_ref[layer, 2:3, :]).astype(BF)
            cast_copy(us_sem, ur_sem, d, i).start()
        reduce(so, ro, os_sem, or_sem, 0, o_end)
        spread(us_sem, ur_sem, 3, None)

        if layer == 0:
            sort_next(t)

            @pl.when(t < 2)
            def _():
                def later(k, _):
                    return q_block(t * blocks + k, 0)
                lax.fori_loop(1, blocks, later, 0)

            @pl.when(t == 1)
            def _():
                wu_load.start()
                load(4, tab_hbm.at[1], tab).start()

        @pl.when(t == 6)
        def _():
            for c in [wg_load, wu_load] + wd_loads:
                c.wait()
        free_stage(sm, rm, ms_sem, mr_sem, 6)

        @pl.when((t >= 6) & (t < n + 9))
        def _():
            for d in (0, 1):
                i = t - 9 + r[d]

                @pl.when((i >= 0) & (i < n) & (r[d] < 3))
                def _():
                    cast_copy(us_sem, ur_sem, d, i).wait_send()

                @pl.when((i >= 0) & (i < n))
                def _():
                    lhs_u[pl.ds(d * C, C), :] = ub[d, jnp.clip(i, 0, n - 1)]

            def hidden(cs):
                gate = jnp.dot(lhs_u[...], wg_v[:, cs], preferred_element_type=F32)
                upper = jnp.dot(lhs_u[...], wu_v[:, cs], preferred_element_type=F32)
                fb[:, cs] = (gate / (1.0 + jnp.exp(-gate)) * upper).astype(BF)

            def hcols(j, _):
                hidden(at(j * 256, 256))
                return 0
            lax.fori_loop(0, ff // 256, hcols, 0, unroll=3)
            if ff % 256:
                hidden(pl.ds(ff // 256 * 256, ff % 256))

            def down_tile(w, j):
                cs = pl.ds(j * 256, 256)
                p = jnp.dot(fb[...], w, preferred_element_type=F32)
                sm[slot, 0, :, cs] = p[:C]
                sm[slot, 1, :, cs] = p[C:]

            def flowing(j):
                k = (t - 6) * flow + j
                wd_tile(k).wait()
                down_tile(wd_b[lax.rem(k, WD_SLOTS)], kept + j)

                @pl.when(k + WD_SLOTS < wd_total)
                def _():
                    wd_tile(k + WD_SLOTS).start()
            for j in range(max(kept, flow)):
                if j < flow:
                    flowing(j)
                if j < kept:
                    down_tile(wd_v[j], j)

        def m_end(d, i):
            ub[d, i] = (hb[i].astype(F32) + rms(sm[slot, d], g_ref[layer, 3:4, :])).astype(BF)
            cast_copy(hs_sem, hr_sem, d, i).start()

            @pl.when(i == n - 1)
            def _():
                for hops in (2, 3):
                    last_copy(d, hops).start()
            out_copy(d, i).start()
        reduce(sm, rm, ms_sem, mr_sem, 6, m_end)
        spread(hs_sem, hr_sem, 9, None if layer == 0 else lambda d, i: out_copy(d, i).start(), n - 1)

        @pl.when(t + 1 < n + 3)
        def _():
            attend(t + 1)

        if layer == 0:
            @pl.when(t == n + 3)
            def _():
                for c in wkv_loads + wq_tiles:
                    c.start()
            first_qkv = n + 12 - pairs

            @pl.when(t == first_qkv)
            def _():
                for c in wkv_loads + [load(4, tab_hbm.at[1], tab)] + wq_tiles:
                    c.wait()

            @pl.when(t >= first_qkv)
            def _():
                next_qkv(t - first_qkv)
        return 0

    lax.fori_loop(0, n + 12, tick, 0)

    if layer == 0:
        forward(pairs - 1)

        @pl.when(s < 3)
        def _():
            halo.wait_send()
            for kind in range(2):
                tail(0, kind).wait_recv()

        @pl.when(s == 3)
        def _():
            for dst in range(3):
                for kind in range(2):
                    tail(dst, kind).wait_send()
            for kind in range(2):
                cache[kind] = kv[2 * kind + 1, pl.ds(rows, WINDOW), :]
        caches = [pltpu.make_async_copy(cache.at[0], kc_hbm, c_sem.at[0]), pltpu.make_async_copy(cache.at[1], vc_hbm, c_sem.at[1])]
        for c in caches:
            c.start()
        for k in (pairs - 2, pairs - 1):
            sent(k)

        def got(k, _):
            for d in range(2):
                kv_pair(d, k).wait_recv()
                kv_fwd(d, k).wait()
            return 0
        lax.fori_loop(0, pairs, got, 0)

    def drain(i, _):
        for d in (0, 1):
            @pl.when((r[d] < 3) & ((i < n - 1) | (r[d] == 0)))
            def _():
                cast_copy(hs_sem, hr_sem, d, i).wait_send()

            @pl.when((r[d] == 0) & (i == n - 1))
            def _():
                for hops in (2, 3):
                    last_copy(d, hops).wait_send()
            if layer == 0:
                @pl.when(r[d] == 0)
                def _():
                    out_copy(d, i).wait()
            else:
                out_copy(d, i).wait()
        return 0
    lax.fori_loop(0, n, drain, 0)
    for c in caches:
        c.wait()


def finish_kernel(parts, *refs):
    k = len(parts)
    ins, outs, bufs, sems = refs[:k], refs[k:2 * k], refs[2 * k:3 * k], refs[3 * k:]
    jobs = []
    for p in range(k):
        size = ins[p].shape[0] // parts[p]
        for e in range(parts[p]):
            cut = pl.ds(e * size, size)
            jobs.append((pltpu.make_async_copy(ins[p].at[cut], bufs[p].at[cut], sems[0].at[len(jobs)]),
                         pltpu.make_async_copy(bufs[p].at[cut], outs[p].at[cut], sems[1].at[len(jobs)])))
    for job in jobs:
        job[0].start()
    for job in jobs:
        job[0].wait()
        job[1].start()
    for job in jobs:
        job[1].wait()


def finish(arrays, parts):
    any_ = pl.BlockSpec(memory_space=pl.ANY)
    dma = pltpu.SemaphoreType.DMA
    return pl.pallas_call(
        functools.partial(finish_kernel, parts),
        out_shape=[jax.ShapeDtypeStruct(a.shape, a.dtype) for a in arrays],
        in_specs=[any_] * len(arrays), out_specs=[any_] * len(arrays),
        scratch_shapes=[pltpu.VMEM(a.shape, a.dtype) for a in arrays] + [dma((sum(parts),)), dma((sum(parts),))],
        compiler_params=pltpu.CompilerParams(vmem_limit_bytes=67043328),
        name='finish',
    )(*arrays)


def run_layer(layer, heads, weights, out_shape):
    dma = pltpu.SemaphoreType.DMA
    any_, vmem = pl.BlockSpec(memory_space=pl.ANY), pl.BlockSpec(memory_space=pltpu.VMEM)
    ka, ff = weights[0].shape[1], weights[1].shape[2]
    C = CHUNK
    n = out_shape[0].shape[-3]
    rows = 2 * n * C
    keys = WINDOW + rows + SPAN - WINDOW if layer == 0 else 4 * rows
    scratch = [
        pltpu.VMEM((ka * D // 256, 256), BF), pltpu.VMEM((D, ff), BF), pltpu.VMEM((D, ff), BF), pltpu.VMEM((WD_KEPT[layer], ff, 256), BF), pltpu.VMEM((WD_SLOTS, ff, 256), BF),
        pltpu.VMEM((2, n, 2, 4 * C, HEAD), BF), pltpu.VMEM((4, keys, HEAD), BF),
        pltpu.VMEM((n, C, D), BF), pltpu.VMEM((2, n, C, D), BF),
        pltpu.VMEM((2, 2, C, D), F32), pltpu.VMEM((2, 2, C, D), F32),
        pltpu.VMEM((2, RING, C, D), F32), pltpu.VMEM((2, RING, C, D), F32),
        pltpu.VMEM((2 * C, ka), BF), pltpu.VMEM((2 * C, D), BF), pltpu.VMEM((2 * C, ff), BF),
        dma((7,)), dma((D // 256,)), dma((WD_KEPT[layer],)), dma((WD_SLOTS,)), dma((2, 2)), dma((2, RING)), dma((2, 2)), dma((2, RING)),
        dma((2, n)), dma((2, n)), dma((2, n)), dma((2, n)), dma((2, 2)), dma((2, n)), dma((2,))]
    if layer == 0:
        p = n // 2
        scratch += [
            pltpu.VMEM((rows, HEAD), F32), pltpu.VMEM((D, 4 * HEAD), BF), pltpu.VMEM((4 * C, D), BF),
            pltpu.VMEM((2, 2, 2, 2, 4 * C, HEAD), BF), pltpu.VMEM((2, 2, 4, 2 * C, HEAD), BF), pltpu.VMEM((2, WINDOW, HEAD), BF),
            pltpu.VMEM((2, 256, 256), BF), pltpu.VMEM((1280, HEAD), BF), pltpu.VMEM((2, 512, HEAD), BF),
            pltpu.VMEM((8, 160, HEAD), BF), pltpu.VMEM((4, 256, HEAD), BF), dma((12,)), dma((3,)), dma((2,)),
            dma((rows // 256,)), dma((8,)), dma((4,)), dma, dma, dma((3, 2)), dma((2,)), dma((2, 2)), dma((2, p)), dma((2, 2)), dma((2, p)), dma((2, 2)),
            dma((2, p)), dma((2, p)), dma((2, 2))]
        in_specs = [any_, vmem] + [any_] * 4
    else:
        scratch += [pltpu.VMEM((2, 2, 3, 4 * C, HEAD), F32), pltpu.VMEM((2, 2, 2, 4 * C, KEYS), F32)]
        in_specs = [any_, any_, any_, vmem]
    return pl.pallas_call(
        functools.partial(layer_kernel, layer),
        out_shape=out_shape,
        in_specs=in_specs + [any_] * 4,
        out_specs=[any_] * len(out_shape),
        scratch_shapes=scratch,
        compiler_params=pltpu.CompilerParams(collective_id=layer, has_side_effects=True, vmem_limit_bytes=67043328),
        cost_estimate=pl.CostEstimate(flops=2 * rows * D * (ka + 3 * ff), bytes_accessed=300_000_000, transcendentals=rows * ff),
        name=f'layer{layer}',
    )(*heads, *weights)


def solution(mesh):
    def device_fn(x, pos, gains, w_q, w_k, w_v, w_o, w_gate, w_up, w_down):
        C = CHUNK
        rows = x.shape[0]
        n = rows // 2 // C
        shape = jax.ShapeDtypeStruct
        wq, wk, wv = (w.reshape(2, -1, HEAD) for w in (w_q, w_k, w_v))
        half = HEAD // 2
        freq = jnp.stack([base ** (-jnp.arange(half, dtype=F32) / half) for base in (LOCAL_BASE, GLOBAL_BASE)])
        grain = 32
        coarse = pos.astype(F32)[::grain][None, :, None] * freq[:, None, :]
        fine = jnp.arange(grain, dtype=F32)[None, :, None] * freq[:, None, :]
        ca, sa, cb, sb = lax.optimization_barrier((jnp.cos(coarse), jnp.sin(coarse), jnp.cos(fine), jnp.sin(fine)))
        ca, sa, cb, sb = ca[:, :, None], sa[:, :, None], cb[:, None], sb[:, None]
        tab = jnp.concatenate([ca * cb - sa * sb, sa * cb + ca * sb], axis=3).reshape(2, rows, HEAD)
        weights = (w_o.reshape(2, 8 * HEAD, D), w_gate, w_up, w_down)
        qshape = shape((2, n, 2, 4 * C, HEAD), BF)
        res, q1, kv1, kl, vl, _, _ = run_layer(
            0, (x.reshape(2, n, C, D), gains, tab, wq, wk, wv), weights,
            [shape((n, C, D), BF), qshape, shape((4, 4 * rows, HEAD), BF), shape((WINDOW, HEAD), BF), shape((WINDOW, HEAD), BF),
             shape((8, D, HEAD), BF), shape((4, D, HEAD), BF)])
        out, kg, vg = run_layer(
            1, (res, q1, kv1, gains), weights,
            [shape((2, n, C, D), BF), shape((4 * rows, HEAD), BF), shape((4 * rows, HEAD), BF)])
        out, kl, vl, kg, vg = finish((out.reshape(rows, D), kl, vl, kg, vg), (8, 1, 1, 2, 2))
        return (out, kl[:, None, :], vl[:, None, :], kg[:, None, :], vg[:, None, :])

    token_spec = P(('rep', 'sp'), None)
    cache_spec = P('rep', ('tp', 'sp'), None)
    in_specs = (token_spec, P(('rep', 'sp')), P(), P(None, None, 'tp', None), P(None, None, 'tp', None),
                P(None, None, 'tp', None), P(None, 'tp', None, None), P(None, None, 'tp'), P(None, None, 'tp'),
                P(None, 'tp', None))
    out_specs = (token_spec, cache_spec, cache_spec, cache_spec, cache_spec)
    return jax.shard_map(device_fn, mesh=mesh, in_specs=in_specs, out_specs=out_specs, check_vma=False)
```
